32 devices in a mesh: gz: 8 (over z, y), gy: 4 (over x, core).
Axes of the slice: x: 2, y: 2, z: 4, core: 2. Of those that a mesh axis runs over, the one named last changes fastest.
Arguments:
- charges: float32 [64, 64, 1024], P('gz', 'gy'), may hold values from -6 to 6
- kernel: float32 [64, 64, 64], P('gz', 'gy'), may hold values from -0.01171875 to 0.01171875
Outputs:
- fine_potential: float32 [128, 128, 2048], P('gz', 'gy')
The draws below stay inside these ranges and needn't reach their ends.
All inputs are finite; a program needn't handle non-finite values.
Results may differ from the reference program's by a relative error of at most 0.000098.
Values sent between devices are 32-bit elements; how exact they have to be, the bound alone decides.
No kernel may reach another device: no remote copies, remote signals or barrier semaphores. Data moves between devices by JAX's collectives and lax.ppermute only.
A program may use at most 128 MiB of HBM per device.

```python
import jax
import jax.numpy as jnp

GRID = 64
REPL = 16
FINE = 128


def block_scale(own_key, shape, cuts, smallest, largest):
    gain = 1.0
    for position, parts in cuts:
        steps = jax.random.uniform(jax.random.fold_in(jax.random.fold_in(own_key, 6), position), (parts,), jnp.float32, smallest / len(cuts), largest / len(cuts))
        gain = gain * jnp.repeat(jnp.exp(steps), shape[position] // parts).reshape((-1,) + (1,) * (len(shape) - 1 - position))
    return gain


def bell_draw(key, shape, width, bound, split=(), held_as=jnp.bfloat16):
    values = jax.random.normal(key, shape, jnp.float32) * width
    if len(split) > 0:
        values = block_scale(key, shape, split, -0.22, 0.18) * values
    return jnp.clip(values, min=-bound, max=bound).astype(held_as)


def setup_inputs(seed: int = 0) -> dict:
    streams_of = jax.random.split(jax.random.key(seed), 3)
    charges = bell_draw(streams_of[0], (GRID, GRID, GRID * REPL), 1.0, 6.0, ((0, 8), (1, 4)), jnp.float32)
    kernel = bell_draw(streams_of[1], (GRID, GRID, GRID), (GRID * GRID * GRID) ** -0.5, 0.01171875, ((0, 8), (1, 4)), jnp.float32)
    return {"charges": charges, "kernel": kernel}


def refine(coarse, axis):
    before = jnp.roll(coarse, 1, axis)
    after = jnp.roll(coarse, -1, axis)
    after_two = jnp.roll(coarse, -2, axis)
    middle = (9.0 * (coarse + after) - (before + after_two)) / 16.0
    stacked = jnp.stack([coarse, middle], axis=axis + 1)
    shape = list(coarse.shape)
    shape[axis] = 2 * shape[axis]
    return stacked.reshape(shape)


def reference(charges, kernel):
    grids = charges.reshape(GRID, GRID, GRID, REPL)
    charge_spec = jnp.fft.fftn(grids, axes=(0, 1, 2))
    kernel_spec = jnp.fft.fftn(kernel, axes=(0, 1, 2))
    potential = jnp.fft.ifftn(charge_spec * kernel_spec[:, :, :, None], axes=(0, 1, 2)).real.astype(jnp.float32)
    result = refine(potential, 0)
    result = refine(result, 1)
    result = refine(result, 2)
    return result.reshape(FINE, FINE, FINE * REPL)
```

```python
import functools
import math

import jax
import jax.numpy as jnp
import numpy as np
from jax import lax
from jax.experimental import pallas as pl
from jax.experimental.pallas import tpu as pltpu
from jax.sharding import PartitionSpec as P

LANES = 128
SUBLANES = 8
TAPS = ((-1, -1.0 / 16.0), (0, 9.0 / 16.0), (1, 9.0 / 16.0), (2, -1.0 / 16.0))
VMEM = pl.BlockSpec(memory_space=pltpu.VMEM)
NT = (((1,), (1,)), ((), ()))
NN = (((1,), (0,)), ((), ()))


class Plan:
    def __init__(self, planes, rows, count, replicas, nz, ny):
        self.planes, self.rows, self.count, self.replicas = planes, rows, count, replicas
        self.nz, self.ny = nz, ny
        self.fine_x = LANES // replicas
        self.radix = count // self.fine_x
        self.parts = nz * ny
        self.block = 2 * replicas
        self.sent = self.block + 2
        self.back = self.block + 3 * self.block // 4
        half = self.radix // 2
        groups = [(0, list(range(0, count // 2, self.radix)))]
        groups.append((half, list(range(half, count // 2, self.radix))))
        for first in range(1, half):
            groups.append((first, list(range(first, count, self.radix))))
        self.groups = groups

    @staticmethod
    def fits(planes, rows, count, replicas, nz, ny):
        if planes * rows != LANES or rows % SUBLANES or 2 * rows * 4 != LANES:
            return False
        if LANES % replicas or replicas % SUBLANES or 2 * replicas != 4 * SUBLANES:
            return False
        fine_x = LANES // replicas
        if count % (2 * fine_x):
            return False
        powers = (count // fine_x, nz, ny, fine_x)
        if any(size & (size - 1) for size in powers):
            return False
        return nz * ny * 2 == count and nz > 2 and ny > 2 and count // fine_x >= 4


def halves(table):
    high = np.asarray(table, np.float32).astype(jnp.bfloat16)
    low = (np.asarray(table, np.float64) - high.astype(np.float64)).astype(jnp.bfloat16)
    return high, low


def side_by_side(table):
    return np.concatenate(halves(table), axis=1)


def spread(small, replicas):
    return np.kron(small, np.eye(replicas))


def slot_rows(plan, modes, at):
    made = []
    for mode in modes:
        angle = 2.0 * np.pi * mode * at / plan.count
        if mode == 0:
            made.append(np.concatenate([np.cos(angle), np.sin(angle)]))
            flip = np.pi * at
            made.append(np.concatenate([np.cos(flip), np.sin(flip)]))
        else:
            made.append(np.concatenate([np.cos(angle), np.sin(angle)]))
            made.append(np.concatenate([-np.sin(angle), np.cos(angle)]))
    return np.stack(made)


def pack_tables(plan):
    at = np.arange(plan.fine_x)
    real, full = [], []
    for first, modes in plan.groups:
        small = slot_rows(plan, modes, at)
        if first in (0, plan.radix // 2):
            real.append(side_by_side(spread(small[:, : plan.fine_x], plan.replicas)))
        else:
            full.append(side_by_side(spread(small, plan.replicas)))
    modes = [mode for _, group in plan.groups for mode in group]
    every = slot_rows(plan, modes, np.arange(plan.count))[:, : plan.count]
    every = np.concatenate([every[0::2], every[1::2]])
    return np.concatenate(real), np.concatenate(full), every.astype(np.float32)


def unpack_tables(plan):
    at = np.arange(plan.fine_x)
    real, full = [], []
    for first, modes in plan.groups:
        rows = slot_rows(plan, modes, at)
        re_of, im_of = rows[:, : plan.fine_x].T, rows[:, plan.fine_x :].T
        if first in (0, plan.radix // 2):
            weight = np.full(re_of.shape, 2.0 / plan.count)
            if first == 0:
                weight[:, :2] = 1.0 / plan.count
            real.append(side_by_side(spread(re_of * weight, plan.replicas)))
        else:
            both = np.concatenate([re_of, im_of]) / plan.count
            full.append(side_by_side(spread(both, plan.replicas)))
    return np.concatenate(real), np.concatenate(full)


def plane_tables(plan):
    count = plan.count
    z_at = np.repeat(np.arange(plan.planes), plan.rows)
    y_at = np.tile(np.arange(plan.rows), plan.planes)
    z_of = np.repeat(np.arange(plan.nz), plan.ny)
    y_of = np.tile(np.arange(plan.ny), plan.nz)
    angle = 2 * np.pi * (np.outer(z_of, z_at) + np.outer(y_of, y_at)) / count
    twist = np.concatenate([np.cos(angle), -np.sin(angle)]).astype(np.float32)
    angle = 2 * np.pi * (np.outer(z_at, z_at) / plan.planes + np.outer(y_at, y_at) / plan.rows)
    cosine, sine = np.cos(angle), np.sin(angle)
    there = np.block([[cosine, -sine], [sine, cosine]])
    scale = 1.0 / (count * count)
    again = np.block([[cosine, sine], [-sine, cosine]]) * scale
    angle = 2 * np.pi * (np.outer(z_of, z_of) / plan.nz + np.outer(y_of, y_of) / plan.ny)
    cosine, sine = np.cos(angle), np.sin(angle)
    blocks = np.block([[cosine, sine], [-sine, cosine], [cosine, -sine], [-sine, -cosine]])
    return twist, side_by_side(there), side_by_side(again), blocks.astype(np.float32)


def halo_moves(plan):
    planes, rows = plan.planes, plan.rows
    quarter = LANES // 4
    taken = {0, 1, planes - 1}
    open_groups = [
        g for g in range(planes)
        if g not in taken and not 2 * quarter <= g * rows < 3 * quarter
    ]
    used = {g: 0 for g in open_groups}
    moves, where = [], {}
    for source, left in (("own", set(range(planes))), ("corner", {planes - 1, 0, 1})):
        while left:
            best = None
            for shift in range(planes):
                for slot in range(rows // 3):
                    hits = [
                        z for z in left
                        if (z + shift) % planes in used and used[(z + shift) % planes] == slot
                    ]
                    if best is None or len(hits) > len(best[2]):
                        best = (shift, slot, hits)
            shift, slot, hits = best
            lanes = []
            for z in hits:
                group = (z + shift) % planes
                used[group] += 1
                left.discard(z)
                plane = z
                if source == "corner":
                    plane = -1 if z == planes - 1 else planes + z
                for step, row in enumerate((rows, rows + 1, -1)):
                    lane = group * rows + 3 * slot + step
                    lanes.append(lane)
                    where[(plane, row)] = lane
            moves.append((source, (shift * rows + 3 * slot) % LANES, tuple(sorted(lanes))))
    for row in range(rows):
        where[(-1, row)] = (planes - 1) * rows + row
        where[(planes, row)] = row
        where[(planes + 1, row)] = rows + row
    return moves, where


def stencil_table(plan):
    _, where = halo_moves(plan)

    def line(size):
        made = np.zeros((2 * size, size + 3))
        for i in range(size):
            made[2 * i, i + 1] = 1.0
            for step, weight in TAPS:
                made[2 * i + 1, i + 1 + step] = weight
        return made

    along_z, along_y = line(plan.planes), line(plan.rows)
    table = np.zeros((4 * plan.planes * plan.rows, 2 * LANES))
    for z in range(-1, plan.planes + 2):
        for y in range(-1, plan.rows + 2):
            if 0 <= z < plan.planes and 0 <= y < plan.rows:
                lane = z * plan.rows + y
            else:
                lane = LANES + where[(z, y)]
            table[:, lane] = np.kron(along_z[:, z + 1], along_y[:, y + 1])
    return table.astype(jnp.bfloat16)


def split(values):
    high = values.astype(jnp.bfloat16)
    low = (values - high.astype(jnp.float32)).astype(jnp.bfloat16)
    return high, low


def dot(a, b, dims):
    return lax.dot_general(a, b, dims, preferred_element_type=jnp.float32)


def dot_exact(a, b, dims):
    return lax.dot_general(
        a, b, dims, precision=lax.Precision.HIGHEST, preferred_element_type=jnp.float32
    )


def add(a, b):
    if a is None:
        return b
    return a if b is None else a + b


def sub(a, b):
    if b is None:
        return a
    return -b if a is None else a - b


def turn(value, angle):
    re, im = value
    c, s = math.cos(angle), math.sin(angle)
    near = 1e-9
    if abs(s) < near:
        return value if c > 0 else (sub(None, re) if re is not None else None, sub(None, im) if im is not None else None)
    if abs(c) < near:
        minus = lambda v: None if v is None else -v
        return (minus(im), re) if s > 0 else (im, minus(re))
    if abs(abs(c) - abs(s)) < near:
        c_sign, s_sign = math.copysign(1.0, c), math.copysign(1.0, s)
        size = abs(c)
        if im is None:
            scaled = re * size
            return (scaled if c_sign > 0 else -scaled, scaled if s_sign > 0 else -scaled)
        first = (re - im) if c_sign * s_sign > 0 else (re + im)
        second = (re + im) if c_sign * s_sign > 0 else (im - re)
        return (first * (c_sign * size), second * (c_sign * size))
    if im is None:
        return (re * c, re * s)
    return (re * c - im * s, re * s + im * c)


def transform(values, sign):
    size = len(values)
    if size == 1:
        return values
    even, odd = transform(values[0::2], sign), transform(values[1::2], sign)
    first, second = [], []
    for k in range(size // 2):
        e, o = even[k], turn(odd[k], sign * 2.0 * math.pi * k / size)
        first.append((add(e[0], o[0]), add(e[1], o[1])))
        second.append((sub(e[0], o[0]), sub(e[1], o[1])))
    return first + second


def from_real(values):
    size = len(values)
    if size == 2:
        return [(values[0] + values[1], None), (values[0] - values[1], None)]
    even, odd = from_real(values[0::2]), from_real(values[1::2])
    made = [None] * (size // 2 + 1)
    for k in range(size // 4 + 1):
        e, o = even[k], turn(odd[k], -2.0 * math.pi * k / size)
        made[k] = (add(e[0], o[0]), add(e[1], o[1]))
        if size // 2 - k != k:
            other = (sub(e[0], o[0]), sub(e[1], o[1]))
            made[size // 2 - k] = (other[0], None if other[1] is None else -other[1])
    made[0] = (made[0][0], None)
    made[size // 2] = (made[size // 2][0], None)
    return made


def to_real(values):
    half = len(values) - 1
    size = 2 * half
    if size == 2:
        a, b = values[0][0], values[1][0]
        return [a + b, a - b]
    even, odd = [], []
    for k in range(half // 2 + 1):
        a = values[k]
        b = values[half - k]
        b = (b[0], None if b[1] is None else -b[1])
        if k == half // 2:
            even.append((a[0] + b[0], None))
            odd.append((turn((None, sub(a[1], b[1])), 2.0 * math.pi * k / size)[0], None))
            continue
        even.append((add(a[0], b[0]), add(a[1], b[1])))
        odd.append(turn((sub(a[0], b[0]), sub(a[1], b[1])), 2.0 * math.pi * k / size))
    made = [None] * size
    made[0::2] = to_real(even)
    made[1::2] = to_real(odd)
    return made


def pack_kernel(plan, charges, kernel, real_table, full_table, kernel_table, out):
    width, block = LANES, plan.block
    tiles = [
        charges[:, :, a * width : (a + 1) * width].reshape(LANES, width)
        for a in range(plan.radix)
    ]
    spectrum = from_real(tiles)
    slot, real_at, full_at = 0, 0, 0
    for first, modes in plan.groups:
        re, im = spectrum[first]
        size = len(modes) * block
        if im is None:
            columns, table, at = width, real_table, real_at
            real_at += size
            values = re
        else:
            columns, table, at = 2 * width, full_table, full_at
            full_at += size
            values = jnp.concatenate([re, im], axis=1)
        high, low = split(values)
        w_high = table[at : at + size, :columns]
        w_low = table[at : at + size, columns:]
        made = dot(
            jnp.concatenate([w_high, w_high, w_low], axis=1),
            jnp.concatenate([high, low, high], axis=1),
            NT,
        )
        for m in range(len(modes)):
            start = (slot + m) * plan.sent
            out[start : start + block, :] = made[m * block : (m + 1) * block]
        slot += len(modes)
    made = dot_exact(kernel_table[...], kernel[...].reshape(LANES, plan.count), NT)
    for c in range(2):
        rows = pl.ds(block + c, plan.parts, stride=plan.sent)
        out[rows, :] = made[c * plan.parts : (c + 1) * plan.parts]


def plane_kernel(
    plan, shared, arrived, twist, there, again, blocks, out,
    first_pass, spectra, gains, high_part, low_part,
):
    nz, ny, parts, reps = plan.nz, plan.ny, plan.parts, plan.replicas
    whole = 2 * LANES

    def both(table):
        high, low = table[:, :whole], table[:, whole:]
        return jnp.concatenate([high, high, low], axis=0)

    def apply(table, size):
        high, low = high_part[:size, :], low_part[:size, :]
        return dot(jnp.concatenate([high, low, high], axis=1), both(table), NN)

    def twisted(re, im, t, sign):
        c = twist[t : t + 1, :]
        s = twist[parts + t : parts + t + 1, :] * sign
        return re * c - im * s, re * s + im * c

    def put(at, size, re, im):
        high, low = split(jnp.concatenate([re, im], axis=1))
        high_part[at : at + size, :] = high
        low_part[at : at + size, :] = low

    lines = jnp.concatenate(
        [arrived[pl.ds(plan.block + c, parts, stride=plan.sent), :] for c in range(2)]
    )
    lines = dot_exact(blocks[...], lines, NN)
    c, s = twist[:parts, :], twist[parts:, :]
    for k in range(2):
        re = lines[2 * k * parts : (2 * k + 1) * parts]
        im = lines[(2 * k + 1) * parts : (2 * k + 2) * parts]
        put(k * parts, parts, re * c - im * s, re * s + im * c)
    made = apply(there, 2 * parts)
    plus_re, plus_im = made[:parts, :LANES], made[:parts, LANES:]
    minus_re, minus_im = made[parts:, :LANES], made[parts:, LANES:]
    a_re, a_im = 0.5 * (plus_re + minus_re), 0.5 * (plus_im + minus_im)
    b_re, b_im = 0.5 * (plus_im - minus_im), 0.5 * (minus_re - plus_re)
    is_shared = shared[0] == 0
    zero = jnp.zeros_like(a_re)
    gains[0 * parts : 1 * parts, :] = jnp.where(is_shared, 0.5 * (a_re + b_re), plus_re)
    gains[1 * parts : 2 * parts, :] = jnp.where(is_shared, 0.5 * (a_im + b_im), plus_im)
    gains[2 * parts : 3 * parts, :] = jnp.where(is_shared, 0.5 * (a_re - b_re), zero)
    gains[3 * parts : 4 * parts, :] = jnp.where(is_shared, 0.5 * (a_im - b_im), zero)

    for gy in range(ny):
        values = []
        for gz in range(nz):
            at = (gz * ny + gy) * plan.sent
            values.append((arrived[at : at + reps, :], arrived[at + reps : at + 2 * reps, :]))
        for kz, (re, im) in enumerate(transform(values, -1)):
            at = (kz * ny + gy) * 2 * reps
            first_pass[at : at + reps, :] = re
            first_pass[at + reps : at + 2 * reps, :] = im
    for kz in range(nz):
        values = []
        for gy in range(ny):
            at = (kz * ny + gy) * 2 * reps
            values.append((first_pass[at : at + reps, :], first_pass[at + reps : at + 2 * reps, :]))
        for ky, (re, im) in enumerate(transform(values, -1)):
            t = kz * ny + ky
            put(t * reps, reps, *twisted(re, im, t, 1.0))
            mirror = (-kz % nz) * ny + (-ky % ny)
            put((parts + mirror) * reps, reps, *twisted(re, -im, mirror, 1.0))
    spectra[...] = apply(there, 2 * parts * reps)

    for t in range(parts):
        u_re, u_im = gains[t : t + 1, :], gains[parts + t : parts + t + 1, :]
        v_re = gains[2 * parts + t : 2 * parts + t + 1, :]
        v_im = gains[3 * parts + t : 3 * parts + t + 1, :]
        at, other = t * reps, (parts + t) * reps
        s_re, s_im = spectra[at : at + reps, :LANES], spectra[at : at + reps, LANES:]
        m_re, m_im = spectra[other : other + reps, :LANES], spectra[other : other + reps, LANES:]
        re = (u_re * s_re - u_im * s_im) + (v_re * m_re - v_im * m_im)
        im = (u_re * s_im + u_im * s_re) + (v_re * m_im + v_im * m_re)
        put(at, reps, re, im)
    spectra[: parts * reps, :] = apply(again, parts * reps)

    for kz in range(nz):
        values = []
        for ky in range(ny):
            t = kz * ny + ky
            at = t * reps
            re, im = spectra[at : at + reps, :LANES], spectra[at : at + reps, LANES:]
            values.append(twisted(re, im, t, -1.0))
        for gy, (re, im) in enumerate(transform(values, 1)):
            at = (kz * ny + gy) * 2 * reps
            first_pass[at : at + reps, :] = re
            first_pass[at + reps : at + 2 * reps, :] = im
    for gy in range(ny):
        values = []
        for kz in range(nz):
            at = (kz * ny + gy) * 2 * reps
            values.append((first_pass[at : at + reps, :], first_pass[at + reps : at + 2 * reps, :]))
        for gz, (re, im) in enumerate(transform(values, 1)):
            at = (gz * ny + gy) * plan.back
            out[at : at + reps, :] = re
            out[at + reps : at + 2 * reps, :] = im

    moves, _ = halo_moves(plan)
    rows, planes = plan.rows, plan.planes
    lane = lax.broadcasted_iota(jnp.int32, (SUBLANES, LANES), 1)
    comb = lane % rows

    def among(lanes):
        mask = lane < 0
        start = None
        for l in list(lanes) + [None]:
            if start is None:
                start, last = l, l
            elif l == last + 1 if l is not None else False:
                last = l
            else:
                mask = mask | ((lane >= start) & (lane <= last))
                start, last = l, l
        return mask

    masks = [among(lanes) for _, _, lanes in moves]
    before_mask = comb == 2
    last_plane = lane >= (planes - 1) * rows
    first_planes = lane < 2 * rows
    quarter = LANES // 4
    spare = (lane >= 2 * quarter) & (lane < 3 * quarter)
    pieces = plan.block // SUBLANES

    def main(gz, gy, piece):
        at = ((gz % nz) * ny + gy % ny) * plan.back + piece * SUBLANES
        return out[at : at + SUBLANES, :]

    def roll(values, shift):
        shift %= LANES
        return values if shift == 0 else pltpu.roll(values, shift, 1)

    for gy in range(ny):
        for piece in range(pieces):
            combs = [
                jnp.where(
                    before_mask,
                    roll(main(gz, gy - 1, piece), 3 - rows),
                    main(gz, gy + 1, piece),
                )
                for gz in range(nz)
            ]
            for gz in range(nz):
                corner = jnp.where(last_plane, combs[gz - 1], combs[(gz + 1) % nz])
                made = None
                for (source, shift, _), mask in zip(moves, masks):
                    moved = roll(combs[gz] if source == "own" else corner, shift)
                    made = moved if made is None else jnp.where(mask, moved, made)
                made = jnp.where(first_planes, main(gz + 1, gy, piece), made)
                made = jnp.where(last_plane, main(gz - 1, gy, piece), made)
                at = ((gz * ny + gy) * pieces + piece) * SUBLANES
                first_pass[at : at + SUBLANES, :] = made
    for s in range(parts):
        extra = first_pass[(s * pieces + pieces - 1) * SUBLANES : (s + 1) * pieces * SUBLANES, :]
        for piece, start in enumerate((0, quarter, 3 * quarter)):
            at = (s * pieces + piece) * SUBLANES
            value = first_pass[at : at + SUBLANES, :]
            to = s * plan.back + plan.block + piece * SUBLANES
            out[to : to + SUBLANES, :] = jnp.where(spare, roll(extra, 2 * quarter - start), value)


def unpack_kernel(
    plan, steps, arrived, real_table, full_table, stencil, out, inside, parts_of, coarse
):
    reps, block = plan.replicas, plan.block
    wide = 2 * LANES
    step = pl.program_id(0)

    @pl.when(step == 0)
    def _():
        lane = lax.broadcasted_iota(jnp.int32, (SUBLANES, LANES), 1)
        quarter = LANES // 4
        slot, real_at, full_at, part_at = 0, 0, 0, 0
        found = {}
        for first, modes in plan.groups:
            for m in range(len(modes)):
                at = (slot + m) * plan.back
                inside[m * block : (m + 1) * block, :LANES] = arrived[at : at + block, :]
                packed = [
                    arrived[at + block + k * SUBLANES : at + block + (k + 1) * SUBLANES, :]
                    for k in range(3)
                ]
                last = jnp.where(
                    lane < quarter,
                    pltpu.roll(packed[0], 2 * quarter, 1),
                    jnp.where(
                        lane < 2 * quarter,
                        pltpu.roll(packed[1], 3 * quarter, 1),
                        pltpu.roll(packed[2], quarter, 1),
                    ),
                )
                for k, value in enumerate(packed + [last]):
                    to = m * block + k * SUBLANES
                    inside[to : to + SUBLANES, LANES:] = value
            depth = len(modes) * block
            high, low = split(inside[:depth, :])
            both = jnp.concatenate([high, low, high], axis=0)
            if first in (0, plan.radix // 2):
                size, table, at = LANES, real_table, real_at
                real_at += size
            else:
                size, table, at = 2 * LANES, full_table, full_at
                full_at += size
            w_high = table[at : at + size, :depth]
            w_low = table[at : at + size, depth:]
            made = dot(jnp.concatenate([w_high, w_high, w_low], axis=1), both, NN)
            parts_of[part_at : part_at + size, :] = made
            found[first] = (part_at, size > LANES)
            part_at += size
            slot += len(modes)
        for x_l in range(plan.fine_x):
            for piece in range(reps // SUBLANES):
                row = x_l * reps + piece * SUBLANES
                values = []
                for first in range(plan.radix // 2 + 1):
                    at, is_full = found[first]
                    re = parts_of[at + row : at + row + SUBLANES, :]
                    im = None
                    if is_full:
                        im = parts_of[at + LANES + row : at + LANES + row + SUBLANES, :]
                    values.append((re, im))
                for xh, value in enumerate(to_real(values)):
                    x = xh * plan.fine_x + x_l
                    places = [x + 1]
                    if x == plan.count - 1:
                        places.append(0)
                    if x < 2:
                        places.append(x + 1 + plan.count)
                    for place in places:
                        to = place * reps + piece * SUBLANES
                        coarse[to : to + SUBLANES, :] = value

    here = plan.count // steps
    made = []
    for i in range(here):
        taps = []
        for move in range(4):
            at = pl.multiple_of((step * here + i + move) * reps, reps)
            taps.append(coarse[pl.ds(at, reps), :])
        made.append(taps[1])
        made.append((taps[1] + taps[2]) * (9.0 / 16.0) - (taps[0] + taps[3]) * (1.0 / 16.0))
    high, low = split(jnp.concatenate(made, axis=0))
    table = stencil[...]
    fine = dot(
        jnp.concatenate([table, table], axis=1), jnp.concatenate([high, low], axis=1), NT
    )
    out[...] = fine.reshape(out.shape)


def exchanged(values, parts):
    rows = values.shape[0]
    values = values.reshape(parts, 1, rows // parts * LANES)
    values = lax.all_to_all(values, ("gz", "gy"), split_axis=0, concat_axis=0, tiled=True)
    return values.reshape(rows, LANES)


def fast_form(plan, charges, kernel):
    f32, bf16 = jnp.float32, jnp.bfloat16
    parts, reps, block = plan.parts, plan.replicas, plan.block
    limit = pltpu.CompilerParams(vmem_limit_bytes=40 * 1024 * 1024)
    tables = [jnp.asarray(t) for t in pack_tables(plan)]
    packed = pl.pallas_call(
        functools.partial(pack_kernel, plan),
        out_shape=jax.ShapeDtypeStruct((parts * plan.sent, LANES), f32),
        in_specs=[VMEM] * 5,
        out_specs=VMEM,
        compiler_params=limit,
        name="pack",
    )(charges, kernel, *tables)
    packed = exchanged(packed, parts)

    me = lax.axis_index("gz") * plan.ny + lax.axis_index("gy")
    tables = [jnp.asarray(t) for t in plane_tables(plan)]
    planes = pl.pallas_call(
        functools.partial(plane_kernel, plan),
        out_shape=jax.ShapeDtypeStruct((parts * plan.back, LANES), f32),
        in_specs=[pl.BlockSpec(memory_space=pltpu.SMEM)] + [VMEM] * 5,
        out_specs=VMEM,
        scratch_shapes=[
            pltpu.VMEM((parts * block, LANES), f32),
            pltpu.VMEM((2 * parts * reps, 2 * LANES), f32),
            pltpu.VMEM((4 * parts, LANES), f32),
            pltpu.VMEM((2 * parts * reps, 2 * LANES), bf16),
            pltpu.VMEM((2 * parts * reps, 2 * LANES), bf16),
        ],
        compiler_params=limit,
        name="plane",
    )(me.reshape(1), packed, *tables)
    planes = exchanged(planes, parts)

    steps = 4
    fine_shape = (2 * plan.planes, 2 * plan.rows, 2 * plan.count * reps)
    tables = [jnp.asarray(t) for t in unpack_tables(plan)]
    fixed = lambda shape: pl.BlockSpec(shape, lambda j: (0,) * len(shape))
    operands = (planes, *tables, jnp.asarray(stencil_table(plan)))
    return pl.pallas_call(
        functools.partial(unpack_kernel, plan, steps),
        out_shape=jax.ShapeDtypeStruct(fine_shape, f32),
        grid=(steps,),
        in_specs=[fixed(o.shape) for o in operands],
        out_specs=pl.BlockSpec(fine_shape[:2] + (fine_shape[2] // steps,), lambda j: (0, 0, j)),
        scratch_shapes=[
            pltpu.VMEM((2 * LANES, 2 * LANES), f32),
            pltpu.VMEM((plan.radix * LANES, 2 * LANES), f32),
            pltpu.VMEM(((plan.count + 3) * reps, 2 * LANES), f32),
        ],
        compiler_params=limit,
        name="unpack",
    )(*operands)


def extended(block, sides, width):
    for axis, dim in sides:
        count = lax.axis_size(axis)
        forward_pairs = [(i, (i + 1) % count) for i in range(count)]
        backward_pairs = [(target, source) for source, target in forward_pairs]
        low = lax.ppermute(
            lax.slice_in_dim(block, block.shape[dim] - width, None, axis=dim), axis, forward_pairs
        )
        high = lax.ppermute(lax.slice_in_dim(block, 0, width, axis=dim), axis, backward_pairs)
        block = jnp.concatenate([low, block, high], axis=dim)
    return block


def tables_of(count):
    index = jnp.arange(count, dtype=jnp.int32)
    product = index[:, None] * index[None, :] % count
    angle = product.astype(jnp.float32) * (2.0 * math.pi / count)
    return (jnp.cos(angle), jnp.sin(angle))


def along(values, table, axis):
    moved = jnp.tensordot(values, table, axes=((axis,), (0,)), precision=lax.Precision.HIGHEST)
    return jnp.moveaxis(moved, -1, axis)


def forward(spectrum, axis, cosines, sines):
    real_part, imag_part = (spectrum[0], spectrum[1])
    inner = axis - 1
    new_real = along(real_part, cosines, inner) + along(imag_part, sines, inner)
    new_imag = along(imag_part, cosines, inner) - along(real_part, sines, inner)
    return jnp.stack([new_real, new_imag])


def backward(spectrum, axis, cosines, sines):
    real_part, imag_part = (spectrum[0], spectrum[1])
    inner = axis - 1
    count = cosines.shape[0]
    new_real = (along(real_part, cosines, inner) - along(imag_part, sines, inner)) / count
    new_imag = (along(imag_part, cosines, inner) + along(real_part, sines, inner)) / count
    return jnp.stack([new_real, new_imag])


def refine_rim(haloed, axis, count):
    centre = lax.slice_in_dim(haloed, 2, 2 + count, axis=axis)
    before = lax.slice_in_dim(haloed, 1, 1 + count, axis=axis)
    after = lax.slice_in_dim(haloed, 3, 3 + count, axis=axis)
    after_two = lax.slice_in_dim(haloed, 4, 4 + count, axis=axis)
    middle = (9.0 * (centre + after) - (before + after_two)) / 16.0
    stacked = jnp.stack([centre, middle], axis=axis + 1)
    shape = list(centre.shape)
    shape[axis] = 2 * count
    return stacked.reshape(shape)


def refine_loop(coarse, axis):
    before = jnp.roll(coarse, 1, axis)
    after = jnp.roll(coarse, -1, axis)
    after_two = jnp.roll(coarse, -2, axis)
    middle = (9.0 * (coarse + after) - (before + after_two)) / 16.0
    stacked = jnp.stack([coarse, middle], axis=axis + 1)
    shape = list(coarse.shape)
    shape[axis] = 2 * shape[axis]
    return stacked.reshape(shape)


def general_form(charges, kernel):
    planes, rows, count = (kernel.shape[0], kernel.shape[1], kernel.shape[2])
    replicas = charges.shape[2] // count
    grids = charges.reshape(planes, rows, count, replicas)
    cosines, sines = tables_of(count)
    spectrum = jnp.stack([along(grids, cosines, 2), -along(grids, sines, 2)])
    kernel_spec = jnp.stack([along(kernel, cosines, 2), -along(kernel, sines, 2)])
    spectrum, kernel_spec = (
        lax.all_to_all(spectrum, "gy", split_axis=3, concat_axis=2, tiled=True),
        lax.all_to_all(kernel_spec, "gy", split_axis=3, concat_axis=2, tiled=True),
    )
    spectrum = forward(spectrum, 2, cosines, sines)
    kernel_spec = forward(kernel_spec, 2, cosines, sines)
    spectrum, kernel_spec = (
        lax.all_to_all(spectrum, "gz", split_axis=2, concat_axis=1, tiled=True),
        lax.all_to_all(kernel_spec, "gz", split_axis=2, concat_axis=1, tiled=True),
    )
    spectrum = forward(spectrum, 1, cosines, sines)
    kernel_spec = forward(kernel_spec, 1, cosines, sines)
    kernel_real = kernel_spec[0][..., None]
    kernel_imag = kernel_spec[1][..., None]
    product_real = spectrum[0] * kernel_real - spectrum[1] * kernel_imag
    product_imag = spectrum[1] * kernel_real + spectrum[0] * kernel_imag
    spectrum = backward(jnp.stack([product_real, product_imag]), 1, cosines, sines)
    spectrum = lax.all_to_all(spectrum, "gz", split_axis=1, concat_axis=2, tiled=True)
    spectrum = backward(spectrum, 2, cosines, sines)
    spectrum = lax.all_to_all(spectrum, "gy", split_axis=2, concat_axis=3, tiled=True)
    potential = (along(spectrum[0], cosines, 2) - along(spectrum[1], sines, 2)) / count
    haloed = extended(potential, (("gz", 0), ("gy", 1)), 2)
    result = refine_rim(haloed, 0, planes)
    result = refine_rim(result, 1, rows)
    result = refine_loop(result, 2)
    return result.reshape(2 * planes, 2 * rows, 2 * count * replicas)


def per_device(nz, ny, charges, kernel):
    planes, rows, count = kernel.shape
    replicas = charges.shape[2] // count
    sizes = (planes, rows, count, replicas, nz, ny)
    if Plan.fits(*sizes):
        return fast_form(Plan(*sizes), charges, kernel)
    return general_form(charges, kernel)


def solution(mesh):
    placed = (P("gz", "gy", None), P("gz", "gy", None))
    sizes = (mesh.shape["gz"], mesh.shape["gy"])
    return jax.shard_map(
        functools.partial(per_device, *sizes),
        mesh=mesh,
        in_specs=placed,
        out_specs=P("gz", "gy", None),
        check_vma=False,
    )
```

```python
import functools
import math

import jax
import jax.numpy as jnp
import numpy as np
from jax import lax
from jax.experimental import pallas as pl
from jax.experimental.pallas import tpu as pltpu
from jax.sharding import PartitionSpec as P

LANES = 128
SUBLANES = 8
TAPS = ((-1, -1.0 / 16.0), (0, 9.0 / 16.0), (1, 9.0 / 16.0), (2, -1.0 / 16.0))
VMEM = pl.BlockSpec(memory_space=pltpu.VMEM)
SMEM = pl.BlockSpec(memory_space=pltpu.SMEM)
HBM = pl.BlockSpec(memory_space=pltpu.HBM)
NT = (((1,), (1,)), ((), ()))
NN = (((1,), (0,)), ((), ()))


class Plan:
    def __init__(self, planes, rows, count, replicas, nz, ny):
        self.planes, self.rows, self.count, self.replicas = planes, rows, count, replicas
        self.nz, self.ny = nz, ny
        self.fine_x = LANES // replicas
        self.radix = count // self.fine_x
        self.parts = nz * ny
        self.block = 2 * replicas
        self.sent = self.block + 2
        self.back = self.block + 3 * self.block // 4
        half = self.radix // 2
        groups = [(0, list(range(0, count // 2, self.radix)))]
        groups.append((half, list(range(half, count // 2, self.radix))))
        for first in range(1, half):
            groups.append((first, list(range(first, count, self.radix))))
        self.groups = groups

    @staticmethod
    def fits(planes, rows, count, replicas, nz, ny):
        if planes * rows != LANES or rows % SUBLANES or 2 * rows * 4 != LANES:
            return False
        if LANES % replicas or replicas % SUBLANES or 2 * replicas != 4 * SUBLANES:
            return False
        fine_x = LANES // replicas
        if count % (2 * fine_x):
            return False
        powers = (count // fine_x, nz, ny, fine_x)
        if any(size & (size - 1) for size in powers):
            return False
        return nz * ny * 2 == count and nz > 2 and ny > 2 and count // fine_x >= 4


def halves(table):
    high = np.asarray(table, np.float32).astype(jnp.bfloat16)
    low = (np.asarray(table, np.float64) - high.astype(np.float64)).astype(jnp.bfloat16)
    return high, low


def side_by_side(table):
    return np.concatenate(halves(table), axis=1)


def spread(small, replicas):
    return np.kron(small, np.eye(replicas))


def slot_rows(plan, modes, at):
    made = []
    for mode in modes:
        angle = 2.0 * np.pi * mode * at / plan.count
        if mode == 0:
            made.append(np.concatenate([np.cos(angle), np.sin(angle)]))
            flip = np.pi * at
            made.append(np.concatenate([np.cos(flip), np.sin(flip)]))
        else:
            made.append(np.concatenate([np.cos(angle), np.sin(angle)]))
            made.append(np.concatenate([-np.sin(angle), np.cos(angle)]))
    return np.stack(made)


def pack_tables(plan):
    at = np.arange(plan.fine_x)
    real, full = [], []
    for first, modes in plan.groups:
        small = slot_rows(plan, modes, at)
        if first in (0, plan.radix // 2):
            real.append(side_by_side(spread(small[:, : plan.fine_x], plan.replicas)))
        else:
            full.append(side_by_side(spread(small, plan.replicas)))
    modes = [mode for _, group in plan.groups for mode in group]
    every = slot_rows(plan, modes, np.arange(plan.count))[:, : plan.count]
    every = np.concatenate([every[0::2], every[1::2]])
    return np.concatenate(real), np.concatenate(full), every.astype(np.float32)


def unpack_tables(plan):
    at = np.arange(plan.fine_x)
    real, full = [], []
    for first, modes in plan.groups:
        rows = slot_rows(plan, modes, at)
        re_of, im_of = rows[:, : plan.fine_x].T, rows[:, plan.fine_x :].T
        if first in (0, plan.radix // 2):
            weight = np.full(re_of.shape, 2.0 / plan.count)
            if first == 0:
                weight[:, :2] = 1.0 / plan.count
            real.append(side_by_side(spread(re_of * weight, plan.replicas)))
        else:
            both = np.concatenate([re_of, im_of]) / plan.count
            full.append(side_by_side(spread(both, plan.replicas)))
    return np.concatenate(real), np.concatenate(full)


def plane_tables(plan):
    count = plan.count
    z_at = np.repeat(np.arange(plan.planes), plan.rows)
    y_at = np.tile(np.arange(plan.rows), plan.planes)
    z_of = np.repeat(np.arange(plan.nz), plan.ny)
    y_of = np.tile(np.arange(plan.ny), plan.nz)
    angle = 2 * np.pi * (np.outer(z_of, z_at) + np.outer(y_of, y_at)) / count
    twist = np.concatenate([np.cos(angle), -np.sin(angle)]).astype(np.float32)
    angle = 2 * np.pi * (np.outer(z_at, z_at) / plan.planes + np.outer(y_at, y_at) / plan.rows)
    cosine, sine = np.cos(angle), np.sin(angle)
    there = np.block([[cosine, -sine], [sine, cosine]])
    scale = 1.0 / (count * count)
    again = np.block([[cosine, sine], [-sine, cosine]]) * scale
    angle = 2 * np.pi * (np.outer(z_of, z_of) / plan.nz + np.outer(y_of, y_of) / plan.ny)
    cosine, sine = np.cos(angle), np.sin(angle)
    blocks = np.block([[cosine, sine], [-sine, cosine], [cosine, -sine], [-sine, -cosine]])
    return twist, blocks.astype(np.float32), side_by_side(there), side_by_side(again)


def halo_moves(plan):
    planes, rows = plan.planes, plan.rows
    quarter = LANES // 4
    taken = {0, 1, planes - 1}
    open_groups = [
        g for g in range(planes)
        if g not in taken and not 2 * quarter <= g * rows < 3 * quarter
    ]
    used = {g: 0 for g in open_groups}
    moves, where = [], {}
    for source, left in (("own", set(range(planes))), ("corner", {planes - 1, 0, 1})):
        while left:
            best = None
            for shift in range(planes):
                for slot in range(rows // 3):
                    hits = [
                        z for z in left
                        if (z + shift) % planes in used and used[(z + shift) % planes] == slot
                    ]
                    if best is None or len(hits) > len(best[2]):
                        best = (shift, slot, hits)
            shift, slot, hits = best
            lanes = []
            for z in hits:
                group = (z + shift) % planes
                used[group] += 1
                left.discard(z)
                plane = z
                if source == "corner":
                    plane = -1 if z == planes - 1 else planes + z
                for step, row in enumerate((rows, rows + 1, -1)):
                    lane = group * rows + 3 * slot + step
                    lanes.append(lane)
                    where[(plane, row)] = lane
            moves.append((source, (shift * rows + 3 * slot) % LANES, tuple(sorted(lanes))))
    for row in range(rows):
        where[(-1, row)] = (planes - 1) * rows + row
        where[(planes, row)] = row
        where[(planes + 1, row)] = rows + row
    return moves, where


def stencil_table(plan):
    _, where = halo_moves(plan)

    def line(size):
        made = np.zeros((2 * size, size + 3))
        for i in range(size):
            made[2 * i, i + 1] = 1.0
            for step, weight in TAPS:
                made[2 * i + 1, i + 1 + step] = weight
        return made

    along_z, along_y = line(plan.planes), line(plan.rows)
    table = np.zeros((4 * plan.planes * plan.rows, 2 * LANES))
    for z in range(-1, plan.planes + 2):
        for y in range(-1, plan.rows + 2):
            if 0 <= z < plan.planes and 0 <= y < plan.rows:
                lane = z * plan.rows + y
            else:
                lane = LANES + where[(z, y)]
            table[:, lane] = np.kron(along_z[:, z + 1], along_y[:, y + 1])
    return table.astype(jnp.bfloat16)


def split(values):
    high = values.astype(jnp.bfloat16)
    low = (values - high.astype(jnp.float32)).astype(jnp.bfloat16)
    return high, low


def dot(a, b, dims):
    return lax.dot_general(a, b, dims, preferred_element_type=jnp.float32)


def dot_exact(a, b, dims):
    return lax.dot_general(
        a, b, dims, precision=lax.Precision.HIGHEST, preferred_element_type=jnp.float32
    )


def add(a, b):
    if a is None:
        return b
    return a if b is None else a + b


def sub(a, b):
    if b is None:
        return a
    return -b if a is None else a - b


def turn(value, angle):
    re, im = value
    c, s = math.cos(angle), math.sin(angle)
    near = 1e-9
    if abs(s) < near:
        return value if c > 0 else (sub(None, re) if re is not None else None, sub(None, im) if im is not None else None)
    if abs(c) < near:
        minus = lambda v: None if v is None else -v
        return (minus(im), re) if s > 0 else (im, minus(re))
    if abs(abs(c) - abs(s)) < near:
        c_sign, s_sign = math.copysign(1.0, c), math.copysign(1.0, s)
        size = abs(c)
        if im is None:
            scaled = re * size
            return (scaled if c_sign > 0 else -scaled, scaled if s_sign > 0 else -scaled)
        first = (re - im) if c_sign * s_sign > 0 else (re + im)
        second = (re + im) if c_sign * s_sign > 0 else (im - re)
        return (first * (c_sign * size), second * (c_sign * size))
    if im is None:
        return (re * c, re * s)
    return (re * c - im * s, re * s + im * c)


def transform(values, sign):
    size = len(values)
    if size == 1:
        return values
    even, odd = transform(values[0::2], sign), transform(values[1::2], sign)
    first, second = [], []
    for k in range(size // 2):
        e, o = even[k], turn(odd[k], sign * 2.0 * math.pi * k / size)
        first.append((add(e[0], o[0]), add(e[1], o[1])))
        second.append((sub(e[0], o[0]), sub(e[1], o[1])))
    return first + second


def from_real(values):
    size = len(values)
    if size == 2:
        return [(values[0] + values[1], None), (values[0] - values[1], None)]
    even, odd = from_real(values[0::2]), from_real(values[1::2])
    made = [None] * (size // 2 + 1)
    for k in range(size // 4 + 1):
        e, o = even[k], turn(odd[k], -2.0 * math.pi * k / size)
        made[k] = (add(e[0], o[0]), add(e[1], o[1]))
        if size // 2 - k != k:
            other = (sub(e[0], o[0]), sub(e[1], o[1]))
            made[size // 2 - k] = (other[0], None if other[1] is None else -other[1])
    made[0] = (made[0][0], None)
    made[size // 2] = (made[size // 2][0], None)
    return made


def to_real(values):
    half = len(values) - 1
    size = 2 * half
    if size == 2:
        a, b = values[0][0], values[1][0]
        return [a + b, a - b]
    even, odd = [], []
    for k in range(half // 2 + 1):
        a = values[k]
        b = values[half - k]
        b = (b[0], None if b[1] is None else -b[1])
        if k == half // 2:
            even.append((a[0] + b[0], None))
            odd.append((turn((None, sub(a[1], b[1])), 2.0 * math.pi * k / size)[0], None))
            continue
        even.append((add(a[0], b[0]), add(a[1], b[1])))
        odd.append(turn((sub(a[0], b[0]), sub(a[1], b[1])), 2.0 * math.pi * k / size))
    made = [None] * size
    made[0::2] = to_real(even)
    made[1::2] = to_real(odd)
    return made


def fetches(sources, targets, arrivals):
    copies = [
        pltpu.make_async_copy(source, target, arrivals.at[i])
        for i, (source, target) in enumerate(zip(sources, targets))
    ]
    for copy in copies:
        copy.start()
    return copies


def room_for(operands):
    return [pltpu.VMEM(o.shape, o.dtype) for o in operands] + [
        pltpu.SemaphoreType.DMA((len(operands),))
    ]


def pack_kernel(plan, ahead, _, *refs):
    sources, later = refs[:5], refs[5 : 5 + ahead]
    out, carried = refs[5 + ahead], refs[6 + ahead : 6 + 2 * ahead]
    targets, arrivals, others = refs[-7:-2], refs[-2], refs[-1]
    copies = fetches(sources, targets, arrivals)
    later_copies = fetches(later, carried, others)
    charges, kernel, real_table, full_table, kernel_table = targets
    width, block = LANES, plan.block
    copies[0].wait()
    tiles = [
        charges[:, :, a * width : (a + 1) * width].reshape(LANES, width)
        for a in range(plan.radix)
    ]
    spectrum = from_real(tiles)
    copies[2].wait()
    slot, real_at, full_at = 0, 0, 0
    for first, modes in plan.groups:
        re, im = spectrum[first]
        size = len(modes) * block
        if im is None:
            columns, table, at = width, real_table, real_at
            real_at += size
            values = re
        else:
            if full_at == 0:
                copies[3].wait()
            columns, table, at = 2 * width, full_table, full_at
            full_at += size
            values = jnp.concatenate([re, im], axis=1)
        high, low = split(values)
        w_high = table[at : at + size, :columns]
        w_low = table[at : at + size, columns:]
        made = dot(
            jnp.concatenate([w_high, w_high, w_low], axis=1),
            jnp.concatenate([high, low, high], axis=1),
            NT,
        )
        for m in range(len(modes)):
            start = (slot + m) * plan.sent
            out[start : start + block, :] = made[m * block : (m + 1) * block]
        slot += len(modes)
    copies[1].wait()
    copies[4].wait()
    made = dot_exact(kernel_table[...], kernel[...].reshape(LANES, plan.count), NT)
    for c in range(2):
        rows = pl.ds(block + c, plan.parts, stride=plan.sent)
        out[rows, :] = made[c * plan.parts : (c + 1) * plan.parts]
    for copy in later_copies:
        copy.wait()


def plane_kernel(plan, ahead, shared, arrived, *refs):
    twist, blocks, there, again = refs[:4]
    later, out, carried = refs[4 : 4 + ahead], refs[4 + ahead], refs[5 + ahead : 5 + 2 * ahead]
    first_pass, spectra, gains, high_part, low_part, others = refs[-6:]
    later_copies = fetches(later, carried, others)
    nz, ny, parts, reps = plan.nz, plan.ny, plan.parts, plan.replicas
    whole = 2 * LANES

    def both(table):
        high, low = table[:, :whole], table[:, whole:]
        return jnp.concatenate([high, high, low], axis=0)

    def apply(table, size):
        high, low = high_part[:size, :], low_part[:size, :]
        return dot(jnp.concatenate([high, low, high], axis=1), both(table), NN)

    def twisted(re, im, t, sign):
        c = twist[t : t + 1, :]
        s = twist[parts + t : parts + t + 1, :] * sign
        return re * c - im * s, re * s + im * c

    def put(at, size, re, im):
        high, low = split(jnp.concatenate([re, im], axis=1))
        high_part[at : at + size, :] = high
        low_part[at : at + size, :] = low

    for gy in range(ny):
        values = []
        for gz in range(nz):
            at = (gz * ny + gy) * plan.sent
            values.append((arrived[at : at + reps, :], arrived[at + reps : at + 2 * reps, :]))
        for kz, (re, im) in enumerate(transform(values, -1)):
            at = (kz * ny + gy) * 2 * reps
            first_pass[at : at + reps, :] = re
            first_pass[at + reps : at + 2 * reps, :] = im
    lines = jnp.concatenate(
        [arrived[pl.ds(plan.block + c, parts, stride=plan.sent), :] for c in range(2)]
    )
    lines = dot_exact(blocks[...], lines, NN)
    c, s = twist[:parts, :], twist[parts:, :]
    for k in range(2):
        re = lines[2 * k * parts : (2 * k + 1) * parts]
        im = lines[(2 * k + 1) * parts : (2 * k + 2) * parts]
        put(k * parts, parts, re * c - im * s, re * s + im * c)
    made = apply(there, 2 * parts)
    plus_re, plus_im = made[:parts, :LANES], made[:parts, LANES:]
    minus_re, minus_im = made[parts:, :LANES], made[parts:, LANES:]
    a_re, a_im = 0.5 * (plus_re + minus_re), 0.5 * (plus_im + minus_im)
    b_re, b_im = 0.5 * (plus_im - minus_im), 0.5 * (minus_re - plus_re)
    is_shared = shared[0] == 0
    zero = jnp.zeros_like(a_re)
    gains[0 * parts : 1 * parts, :] = jnp.where(is_shared, 0.5 * (a_re + b_re), plus_re)
    gains[1 * parts : 2 * parts, :] = jnp.where(is_shared, 0.5 * (a_im + b_im), plus_im)
    gains[2 * parts : 3 * parts, :] = jnp.where(is_shared, 0.5 * (a_re - b_re), zero)
    gains[3 * parts : 4 * parts, :] = jnp.where(is_shared, 0.5 * (a_im - b_im), zero)

    for kz in range(nz):
        values = []
        for gy in range(ny):
            at = (kz * ny + gy) * 2 * reps
            values.append((first_pass[at : at + reps, :], first_pass[at + reps : at + 2 * reps, :]))
        for ky, (re, im) in enumerate(transform(values, -1)):
            t = kz * ny + ky
            put(t * reps, reps, *twisted(re, im, t, 1.0))
            mirror = (-kz % nz) * ny + (-ky % ny)
            put((parts + mirror) * reps, reps, *twisted(re, -im, mirror, 1.0))
    spectra[...] = apply(there, 2 * parts * reps)

    for t in range(parts):
        u_re, u_im = gains[t : t + 1, :], gains[parts + t : parts + t + 1, :]
        v_re = gains[2 * parts + t : 2 * parts + t + 1, :]
        v_im = gains[3 * parts + t : 3 * parts + t + 1, :]
        at, other = t * reps, (parts + t) * reps
        s_re, s_im = spectra[at : at + reps, :LANES], spectra[at : at + reps, LANES:]
        m_re, m_im = spectra[other : other + reps, :LANES], spectra[other : other + reps, LANES:]
        re = (u_re * s_re - u_im * s_im) + (v_re * m_re - v_im * m_im)
        im = (u_re * s_im + u_im * s_re) + (v_re * m_im + v_im * m_re)
        put(at, reps, re, im)
    spectra[: parts * reps, :] = apply(again, parts * reps)

    for kz in range(nz):
        values = []
        for ky in range(ny):
            t = kz * ny + ky
            at = t * reps
            re, im = spectra[at : at + reps, :LANES], spectra[at : at + reps, LANES:]
            values.append(twisted(re, im, t, -1.0))
        for gy, (re, im) in enumerate(transform(values, 1)):
            at = (kz * ny + gy) * 2 * reps
            first_pass[at : at + reps, :] = re
            first_pass[at + reps : at + 2 * reps, :] = im
    for gy in range(ny):
        values = []
        for kz in range(nz):
            at = (kz * ny + gy) * 2 * reps
            values.append((first_pass[at : at + reps, :], first_pass[at + reps : at + 2 * reps, :]))
        for gz, (re, im) in enumerate(transform(values, 1)):
            at = (gz * ny + gy) * plan.back
            out[at : at + reps, :] = re
            out[at + reps : at + 2 * reps, :] = im

    moves, _ = halo_moves(plan)
    rows, planes = plan.rows, plan.planes
    lane = lax.broadcasted_iota(jnp.int32, (SUBLANES, LANES), 1)
    comb = lane % rows

    def among(lanes):
        mask = lane < 0
        start = None
        for l in list(lanes) + [None]:
            if start is None:
                start, last = l, l
            elif l == last + 1 if l is not None else False:
                last = l
            else:
                mask = mask | ((lane >= start) & (lane <= last))
                start, last = l, l
        return mask

    masks = [among(lanes) for _, _, lanes in moves]
    before_mask = comb == 2
    last_plane = lane >= (planes - 1) * rows
    first_planes = lane < 2 * rows
    quarter = LANES // 4
    spare = (lane >= 2 * quarter) & (lane < 3 * quarter)
    pieces = plan.block // SUBLANES

    def main(gz, gy, piece):
        at = ((gz % nz) * ny + gy % ny) * plan.back + piece * SUBLANES
        return out[at : at + SUBLANES, :]

    def roll(values, shift):
        shift %= LANES
        return values if shift == 0 else pltpu.roll(values, shift, 1)

    for gy in range(ny):
        for piece in range(pieces):
            combs = [
                jnp.where(
                    before_mask,
                    roll(main(gz, gy - 1, piece), 3 - rows),
                    main(gz, gy + 1, piece),
                )
                for gz in range(nz)
            ]
            for gz in range(nz):
                corner = jnp.where(last_plane, combs[gz - 1], combs[(gz + 1) % nz])
                made = None
                for (source, shift, _), mask in zip(moves, masks):
                    moved = roll(combs[gz] if source == "own" else corner, shift)
                    made = moved if made is None else jnp.where(mask, moved, made)
                made = jnp.where(first_planes, main(gz + 1, gy, piece), made)
                made = jnp.where(last_plane, main(gz - 1, gy, piece), made)
                at = ((gz * ny + gy) * pieces + piece) * SUBLANES
                first_pass[at : at + SUBLANES, :] = made
    for s in range(parts):
        extra = first_pass[(s * pieces + pieces - 1) * SUBLANES : (s + 1) * pieces * SUBLANES, :]
        for piece, start in enumerate((0, quarter, 3 * quarter)):
            at = (s * pieces + piece) * SUBLANES
            value = first_pass[at : at + SUBLANES, :]
            to = s * plan.back + plan.block + piece * SUBLANES
            out[to : to + SUBLANES, :] = jnp.where(spare, roll(extra, 2 * quarter - start), value)
    for copy in later_copies:
        copy.wait()


def unpack_kernel(
    plan, steps, arrived, real_table, full_table, stencil, out, inside, parts_of, coarse
):
    reps, block = plan.replicas, plan.block
    wide = 2 * LANES
    step = pl.program_id(0)

    @pl.when(step == 0)
    def _():
        lane = lax.broadcasted_iota(jnp.int32, (SUBLANES, LANES), 1)
        quarter = LANES // 4
        slot, real_at, full_at, part_at = 0, 0, 0, 0
        found = {}
        for first, modes in plan.groups:
            for m in range(len(modes)):
                at = (slot + m) * plan.back
                inside[m * block : (m + 1) * block, :LANES] = arrived[at : at + block, :]
                packed = [
                    arrived[at + block + k * SUBLANES : at + block + (k + 1) * SUBLANES, :]
                    for k in range(3)
                ]
                last = jnp.where(
                    lane < quarter,
                    pltpu.roll(packed[0], 2 * quarter, 1),
                    jnp.where(
                        lane < 2 * quarter,
                        pltpu.roll(packed[1], 3 * quarter, 1),
                        pltpu.roll(packed[2], quarter, 1),
                    ),
                )
                for k, value in enumerate(packed + [last]):
                    to = m * block + k * SUBLANES
                    inside[to : to + SUBLANES, LANES:] = value
            depth = len(modes) * block
            high, low = split(inside[:depth, :])
            both = jnp.concatenate([high, low, high], axis=0)
            if first in (0, plan.radix // 2):
                size, table, at = LANES, real_table, real_at
                real_at += size
            else:
                size, table, at = 2 * LANES, full_table, full_at
                full_at += size
            w_high = table[at : at + size, :depth]
            w_low = table[at : at + size, depth:]
            made = dot(jnp.concatenate([w_high, w_high, w_low], axis=1), both, NN)
            parts_of[part_at : part_at + size, :] = made
            found[first] = (part_at, size > LANES)
            part_at += size
            slot += len(modes)
        for x_l in range(plan.fine_x):
            for piece in range(reps // SUBLANES):
                row = x_l * reps + piece * SUBLANES
                values = []
                for first in range(plan.radix // 2 + 1):
                    at, is_full = found[first]
                    re = parts_of[at + row : at + row + SUBLANES, :]
                    im = None
                    if is_full:
                        im = parts_of[at + LANES + row : at + LANES + row + SUBLANES, :]
                    values.append((re, im))
                for xh, value in enumerate(to_real(values)):
                    x = xh * plan.fine_x + x_l
                    places = [x + 1]
                    if x == plan.count - 1:
                        places.append(0)
                    if x < 2:
                        places.append(x + 1 + plan.count)
                    for place in places:
                        to = place * reps + piece * SUBLANES
                        coarse[to : to + SUBLANES, :] = value

    here = plan.count // steps
    made = []
    for i in range(here):
        taps = []
        for move in range(4):
            at = pl.multiple_of((step * here + i + move) * reps, reps)
            taps.append(coarse[pl.ds(at, reps), :])
        made.append(taps[1])
        made.append((taps[1] + taps[2]) * (9.0 / 16.0) - (taps[0] + taps[3]) * (1.0 / 16.0))
    high, low = split(jnp.concatenate(made, axis=0))
    table = stencil[...]
    fine = dot(
        jnp.concatenate([table, table], axis=1), jnp.concatenate([high, low], axis=1), NT
    )
    out[...] = fine.reshape(out.shape)


def exchanged(values, parts):
    rows = values.shape[0]
    values = values.reshape(parts, 1, rows // parts * LANES)
    values = lax.all_to_all(values, ("gz", "gy"), split_axis=0, concat_axis=0, tiled=True)
    return values.reshape(rows, LANES)


def in_hbm(arrays):
    return [pltpu.with_memory_space_constraint(array, pltpu.HBM) for array in arrays]


def like(arrays):
    return [jax.ShapeDtypeStruct(array.shape, array.dtype) for array in arrays]


def fast_form(plan, charges, kernel):
    f32, bf16 = jnp.float32, jnp.bfloat16
    parts, reps, block = plan.parts, plan.replicas, plan.block
    limit = pltpu.CompilerParams(vmem_limit_bytes=40 * 1024 * 1024)
    me = (lax.axis_index("gz") * plan.ny + lax.axis_index("gy")).reshape(1)

    operands = [charges, kernel] + [jnp.asarray(t) for t in pack_tables(plan)]
    tables = [jnp.asarray(t) for t in plane_tables(plan)]
    packed, *tables = pl.pallas_call(
        functools.partial(pack_kernel, plan, len(tables)),
        out_shape=[jax.ShapeDtypeStruct((parts * plan.sent, LANES), f32)] + like(tables),
        in_specs=[SMEM] + [HBM] * (len(operands) + len(tables)),
        out_specs=[VMEM] * (1 + len(tables)),
        scratch_shapes=room_for(operands) + [pltpu.SemaphoreType.DMA((len(tables),))],
        compiler_params=limit,
        name="pack",
    )(me, *in_hbm(operands), *in_hbm(tables))
    packed = exchanged(packed, parts)

    later = [jnp.asarray(t) for t in unpack_tables(plan) + (stencil_table(plan),)]
    planes, *later = pl.pallas_call(
        functools.partial(plane_kernel, plan, len(later)),
        out_shape=[jax.ShapeDtypeStruct((parts * plan.back, LANES), f32)] + like(later),
        in_specs=[SMEM] + [VMEM] * (1 + len(tables)) + [HBM] * len(later),
        out_specs=[VMEM] * (1 + len(later)),
        scratch_shapes=[
            pltpu.VMEM((parts * block, LANES), f32),
            pltpu.VMEM((2 * parts * reps, 2 * LANES), f32),
            pltpu.VMEM((4 * parts, LANES), f32),
            pltpu.VMEM((2 * parts * reps, 2 * LANES), bf16),
            pltpu.VMEM((2 * parts * reps, 2 * LANES), bf16),
            pltpu.SemaphoreType.DMA((len(later),)),
        ],
        compiler_params=limit,
        name="plane",
    )(me, packed, *tables, *in_hbm(later))
    planes = exchanged(planes, parts)

    steps = 4
    fine_shape = (2 * plan.planes, 2 * plan.rows, 2 * plan.count * reps)
    fixed = lambda shape: pl.BlockSpec(shape, lambda j: (0,) * len(shape))
    operands = (planes, *later)
    return pl.pallas_call(
        functools.partial(unpack_kernel, plan, steps),
        out_shape=jax.ShapeDtypeStruct(fine_shape, f32),
        grid=(steps,),
        in_specs=[fixed(o.shape) for o in operands],
        out_specs=pl.BlockSpec(fine_shape[:2] + (fine_shape[2] // steps,), lambda j: (0, 0, j)),
        scratch_shapes=[
            pltpu.VMEM((2 * LANES, 2 * LANES), f32),
            pltpu.VMEM((plan.radix * LANES, 2 * LANES), f32),
            pltpu.VMEM(((plan.count + 3) * reps, 2 * LANES), f32),
        ],
        compiler_params=limit,
        name="unpack",
    )(*operands)


def extended(block, sides, width):
    for axis, dim in sides:
        count = lax.axis_size(axis)
        forward_pairs = [(i, (i + 1) % count) for i in range(count)]
        backward_pairs = [(target, source) for source, target in forward_pairs]
        low = lax.ppermute(
            lax.slice_in_dim(block, block.shape[dim] - width, None, axis=dim), axis, forward_pairs
        )
        high = lax.ppermute(lax.slice_in_dim(block, 0, width, axis=dim), axis, backward_pairs)
        block = jnp.concatenate([low, block, high], axis=dim)
    return block


def tables_of(count):
    index = jnp.arange(count, dtype=jnp.int32)
    product = index[:, None] * index[None, :] % count
    angle = product.astype(jnp.float32) * (2.0 * math.pi / count)
    return (jnp.cos(angle), jnp.sin(angle))


def along(values, table, axis):
    moved = jnp.tensordot(values, table, axes=((axis,), (0,)), precision=lax.Precision.HIGHEST)
    return jnp.moveaxis(moved, -1, axis)


def forward(spectrum, axis, cosines, sines):
    real_part, imag_part = (spectrum[0], spectrum[1])
    inner = axis - 1
    new_real = along(real_part, cosines, inner) + along(imag_part, sines, inner)
    new_imag = along(imag_part, cosines, inner) - along(real_part, sines, inner)
    return jnp.stack([new_real, new_imag])


def backward(spectrum, axis, cosines, sines):
    real_part, imag_part = (spectrum[0], spectrum[1])
    inner = axis - 1
    count = cosines.shape[0]
    new_real = (along(real_part, cosines, inner) - along(imag_part, sines, inner)) / count
    new_imag = (along(imag_part, cosines, inner) + along(real_part, sines, inner)) / count
    return jnp.stack([new_real, new_imag])


def refine_rim(haloed, axis, count):
    centre = lax.slice_in_dim(haloed, 2, 2 + count, axis=axis)
    before = lax.slice_in_dim(haloed, 1, 1 + count, axis=axis)
    after = lax.slice_in_dim(haloed, 3, 3 + count, axis=axis)
    after_two = lax.slice_in_dim(haloed, 4, 4 + count, axis=axis)
    middle = (9.0 * (centre + after) - (before + after_two)) / 16.0
    stacked = jnp.stack([centre, middle], axis=axis + 1)
    shape = list(centre.shape)
    shape[axis] = 2 * count
    return stacked.reshape(shape)


def refine_loop(coarse, axis):
    before = jnp.roll(coarse, 1, axis)
    after = jnp.roll(coarse, -1, axis)
    after_two = jnp.roll(coarse, -2, axis)
    middle = (9.0 * (coarse + after) - (before + after_two)) / 16.0
    stacked = jnp.stack([coarse, middle], axis=axis + 1)
    shape = list(coarse.shape)
    shape[axis] = 2 * shape[axis]
    return stacked.reshape(shape)


def general_form(charges, kernel):
    planes, rows, count = (kernel.shape[0], kernel.shape[1], kernel.shape[2])
    replicas = charges.shape[2] // count
    grids = charges.reshape(planes, rows, count, replicas)
    cosines, sines = tables_of(count)
    spectrum = jnp.stack([along(grids, cosines, 2), -along(grids, sines, 2)])
    kernel_spec = jnp.stack([along(kernel, cosines, 2), -along(kernel, sines, 2)])
    spectrum, kernel_spec = (
        lax.all_to_all(spectrum, "gy", split_axis=3, concat_axis=2, tiled=True),
        lax.all_to_all(kernel_spec, "gy", split_axis=3, concat_axis=2, tiled=True),
    )
    spectrum = forward(spectrum, 2, cosines, sines)
    kernel_spec = forward(kernel_spec, 2, cosines, sines)
    spectrum, kernel_spec = (
        lax.all_to_all(spectrum, "gz", split_axis=2, concat_axis=1, tiled=True),
        lax.all_to_all(kernel_spec, "gz", split_axis=2, concat_axis=1, tiled=True),
    )
    spectrum = forward(spectrum, 1, cosines, sines)
    kernel_spec = forward(kernel_spec, 1, cosines, sines)
    kernel_real = kernel_spec[0][..., None]
    kernel_imag = kernel_spec[1][..., None]
    product_real = spectrum[0] * kernel_real - spectrum[1] * kernel_imag
    product_imag = spectrum[1] * kernel_real + spectrum[0] * kernel_imag
    spectrum = backward(jnp.stack([product_real, product_imag]), 1, cosines, sines)
    spectrum = lax.all_to_all(spectrum, "gz", split_axis=1, concat_axis=2, tiled=True)
    spectrum = backward(spectrum, 2, cosines, sines)
    spectrum = lax.all_to_all(spectrum, "gy", split_axis=2, concat_axis=3, tiled=True)
    potential = (along(spectrum[0], cosines, 2) - along(spectrum[1], sines, 2)) / count
    haloed = extended(potential, (("gz", 0), ("gy", 1)), 2)
    result = refine_rim(haloed, 0, planes)
    result = refine_rim(result, 1, rows)
    result = refine_loop(result, 2)
    return result.reshape(2 * planes, 2 * rows, 2 * count * replicas)


def per_device(nz, ny, charges, kernel):
    planes, rows, count = kernel.shape
    replicas = charges.shape[2] // count
    sizes = (planes, rows, count, replicas, nz, ny)
    if Plan.fits(*sizes):
        return fast_form(Plan(*sizes), charges, kernel)
    return general_form(charges, kernel)


def solution(mesh):
    placed = (P("gz", "gy", None), P("gz", "gy", None))
    sizes = (mesh.shape["gz"], mesh.shape["gy"])
    return jax.shard_map(
        functools.partial(per_device, *sizes),
        mesh=mesh,
        in_specs=placed,
        out_specs=P("gz", "gy", None),
        check_vma=False,
    )
```

```python
import functools
import math

import jax
import jax.numpy as jnp
import numpy as np
from jax import lax
from jax.experimental import pallas as pl
from jax.experimental.pallas import tpu as pltpu
from jax.sharding import PartitionSpec as P

LANES = 128
SUBLANES = 8
TAPS = ((-1, -1.0 / 16.0), (0, 9.0 / 16.0), (1, 9.0 / 16.0), (2, -1.0 / 16.0))
VMEM = pl.BlockSpec(memory_space=pltpu.VMEM)
SMEM = pl.BlockSpec(memory_space=pltpu.SMEM)
HBM = pl.BlockSpec(memory_space=pltpu.HBM)
NT = (((1,), (1,)), ((), ()))
NN = (((1,), (0,)), ((), ()))


class Plan:
    def __init__(self, planes, rows, count, replicas, nz, ny):
        self.planes, self.rows, self.count, self.replicas = planes, rows, count, replicas
        self.nz, self.ny = nz, ny
        self.fine_x = LANES // replicas
        self.radix = count // self.fine_x
        self.parts = nz * ny
        self.block = 2 * replicas
        self.sent = self.block + 2
        self.back = self.block + 3 * self.block // 4
        half = self.radix // 2
        groups = [(0, list(range(0, count // 2, self.radix)))]
        groups.append((half, list(range(half, count // 2, self.radix))))
        for first in range(1, half):
            groups.append((first, list(range(first, count, self.radix))))
        self.groups = groups

    @staticmethod
    def fits(planes, rows, count, replicas, nz, ny):
        if planes * rows != LANES or rows % SUBLANES or 2 * rows * 4 != LANES:
            return False
        if LANES % replicas or replicas % SUBLANES or 2 * replicas != 4 * SUBLANES:
            return False
        fine_x = LANES // replicas
        if count % (2 * fine_x):
            return False
        powers = (count // fine_x, nz, ny, fine_x)
        if any(size & (size - 1) for size in powers):
            return False
        return nz * ny * 2 == count and nz > 2 and ny > 2 and count // fine_x >= 4


def halves(table):
    high = np.asarray(table, np.float32).astype(jnp.bfloat16)
    low = (np.asarray(table, np.float64) - high.astype(np.float64)).astype(jnp.bfloat16)
    return high, low


def side_by_side(table):
    return np.concatenate(halves(table), axis=1)


def spread(small, replicas):
    return np.kron(small, np.eye(replicas))


def slot_rows(plan, modes, at, shared=True):
    made = []
    for mode in modes:
        angle = 2.0 * np.pi * mode * at / plan.count
        if shared and mode == 0:
            made.append(np.concatenate([np.cos(angle), np.sin(angle)]))
            flip = np.pi * at
            made.append(np.concatenate([np.cos(flip), np.sin(flip)]))
        else:
            made.append(np.concatenate([np.cos(angle), np.sin(angle)]))
            made.append(np.concatenate([-np.sin(angle), np.cos(angle)]))
    return np.stack(made)


def shared_slot(plan, table):
    half = plan.replicas // 2
    order = [
        (j // half) * plan.replicas + j % half + half * c
        for c in range(2)
        for j in range(plan.replicas)
    ]
    return np.concatenate([table[order], table[plan.block :]])


def full_rows(plan):
    modes = range(0, plan.count, plan.radix)
    return slot_rows(plan, modes, np.arange(plan.fine_x), shared=False)


def pack_tables(plan):
    at = np.arange(plan.fine_x)
    real = []
    for first, modes in plan.groups[:2]:
        table = spread(slot_rows(plan, modes, at)[:, : plan.fine_x], plan.replicas)
        real.append(side_by_side(shared_slot(plan, table) if first == 0 else table))
    turns = np.zeros((2 * plan.radix, LANES))
    for first in range(plan.radix):
        angle = np.repeat(2.0 * np.pi * first * at / plan.count, plan.replicas)
        turns[first], turns[plan.radix + first] = np.cos(angle), -np.sin(angle)
    modes = [mode for _, group in plan.groups for mode in group]
    every = slot_rows(plan, modes, np.arange(plan.count))[:, : plan.count]
    every = np.concatenate([every[0::2], every[1::2]])
    full = side_by_side(spread(full_rows(plan), plan.replicas))
    single = np.float32
    return np.concatenate(real), full, every.astype(single), turns.astype(single)


def unpack_tables(plan):
    at = np.arange(plan.fine_x)
    real = []
    for first, modes in plan.groups[:2]:
        re_of = slot_rows(plan, modes, at)[:, : plan.fine_x].T
        weight = np.full(re_of.shape, 2.0 / plan.count)
        if first == 0:
            weight[:, :2] = 1.0 / plan.count
        table = spread(re_of * weight, plan.replicas)
        real.append(side_by_side(shared_slot(plan, table.T).T if first == 0 else table))
    full = side_by_side(spread(full_rows(plan).T / plan.count, plan.replicas))
    return np.concatenate(real), full


def plane_tables(plan):
    count = plan.count
    z_at = np.repeat(np.arange(plan.planes), plan.rows)
    y_at = np.tile(np.arange(plan.rows), plan.planes)
    z_of = np.repeat(np.arange(plan.nz), plan.ny)
    y_of = np.tile(np.arange(plan.ny), plan.nz)
    angle = 2 * np.pi * (np.outer(z_of, z_at) + np.outer(y_of, y_at)) / count
    twist = np.concatenate([np.cos(angle), -np.sin(angle)]).astype(np.float32)
    angle = 2 * np.pi * (np.outer(z_at, z_at) / plan.planes + np.outer(y_at, y_at) / plan.rows)
    cosine, sine = np.cos(angle), np.sin(angle)
    there = np.block([[cosine, -sine], [sine, cosine]])
    angle = 2 * np.pi * (np.outer(z_of, z_of) / plan.nz + np.outer(y_of, y_of) / plan.ny)
    cosine, sine = np.cos(angle), np.sin(angle)
    blocks = np.block([[cosine, sine], [-sine, cosine], [cosine, -sine], [-sine, -cosine]])
    return twist, blocks.astype(np.float32), side_by_side(there), side_table(plan)


def halo_places(plan):
    planes, rows = plan.planes, plan.rows
    quarter = LANES // 4
    open_lanes = [
        lane
        for lane in range(2 * rows, (planes - 1) * rows)
        if not 2 * quarter <= lane < 3 * quarter
    ]
    sides = [(z, y) for z in range(-1, planes + 2) for y in (-1, rows, rows + 1)]
    places = dict(zip(sides, open_lanes, strict=False))
    for row in range(rows):
        places[(-1, row)] = (planes - 1) * rows + row
        places[(planes, row)] = row
        places[(planes + 1, row)] = rows + row
    return places


def side_table(plan):
    planes, rows = plan.planes, plan.rows
    table = np.zeros((2 * LANES, LANES))
    for (z, y), lane in halo_places(plan).items():
        if 0 <= y < rows:
            continue
        source = z % planes * rows + y % rows
        table[source if 0 <= z < planes else LANES + source, lane] = 1.0
    return table.astype(jnp.bfloat16)


def stencil_table(plan):
    where = halo_places(plan)

    def line(size):
        made = np.zeros((2 * size, size + 3))
        for i in range(size):
            made[2 * i, i + 1] = 1.0
            for step, weight in TAPS:
                made[2 * i + 1, i + 1 + step] = weight
        return made

    along_z, along_y = np.eye(plan.planes + 3), line(plan.rows)
    table = np.zeros((2 * (plan.planes + 3) * plan.rows, 2 * LANES))
    for z in range(-1, plan.planes + 2):
        for y in range(-1, plan.rows + 2):
            if 0 <= z < plan.planes and 0 <= y < plan.rows:
                lane = z * plan.rows + y
            else:
                lane = LANES + where[(z, y)]
            table[:, lane] = np.kron(along_z[:, z + 1], along_y[:, y + 1])
    return table.astype(jnp.bfloat16)


def split(values):
    high = values.astype(jnp.bfloat16)
    low = (values - high.astype(jnp.float32)).astype(jnp.bfloat16)
    return high, low


def dot(a, b, dims):
    return lax.dot_general(a, b, dims, preferred_element_type=jnp.float32)


def dot_exact(a, b, dims):
    return lax.dot_general(
        a, b, dims, precision=lax.Precision.HIGHEST, preferred_element_type=jnp.float32
    )


def add(a, b):
    if a is None:
        return b
    return a if b is None else a + b


def sub(a, b):
    if b is None:
        return a
    return -b if a is None else a - b


def turn(value, angle):
    re, im = value
    c, s = math.cos(angle), math.sin(angle)
    near = 1e-9
    if abs(s) < near:
        return value if c > 0 else (sub(None, re) if re is not None else None, sub(None, im) if im is not None else None)
    if abs(c) < near:
        minus = lambda v: None if v is None else -v
        return (minus(im), re) if s > 0 else (im, minus(re))
    if abs(abs(c) - abs(s)) < near:
        c_sign, s_sign = math.copysign(1.0, c), math.copysign(1.0, s)
        size = abs(c)
        if im is None:
            scaled = re * size
            return (scaled if c_sign > 0 else -scaled, scaled if s_sign > 0 else -scaled)
        first = (re - im) if c_sign * s_sign > 0 else (re + im)
        second = (re + im) if c_sign * s_sign > 0 else (im - re)
        return (first * (c_sign * size), second * (c_sign * size))
    if im is None:
        return (re * c, re * s)
    return (re * c - im * s, re * s + im * c)


def transform(values, sign):
    size = len(values)
    if size == 1:
        return values
    even, odd = transform(values[0::2], sign), transform(values[1::2], sign)
    first, second = [], []
    for k in range(size // 2):
        e, o = even[k], turn(odd[k], sign * 2.0 * math.pi * k / size)
        first.append((add(e[0], o[0]), add(e[1], o[1])))
        second.append((sub(e[0], o[0]), sub(e[1], o[1])))
    return first + second


def from_real(values):
    size = len(values)
    if size == 2:
        return [(values[0] + values[1], None), (values[0] - values[1], None)]
    even, odd = from_real(values[0::2]), from_real(values[1::2])
    made = [None] * (size // 2 + 1)
    for k in range(size // 4 + 1):
        e, o = even[k], turn(odd[k], -2.0 * math.pi * k / size)
        made[k] = (add(e[0], o[0]), add(e[1], o[1]))
        if size // 2 - k != k:
            other = (sub(e[0], o[0]), sub(e[1], o[1]))
            made[size // 2 - k] = (other[0], None if other[1] is None else -other[1])
    made[0] = (made[0][0], None)
    made[size // 2] = (made[size // 2][0], None)
    return made


def to_real(values):
    half = len(values) - 1
    size = 2 * half
    if size == 2:
        a, b = values[0][0], values[1][0]
        return [a + b, a - b]
    even, odd = [], []
    for k in range(half // 2 + 1):
        a = values[k]
        b = values[half - k]
        b = (b[0], None if b[1] is None else -b[1])
        if k == half // 2:
            even.append((a[0] + b[0], None))
            odd.append((turn((None, sub(a[1], b[1])), 2.0 * math.pi * k / size)[0], None))
            continue
        even.append((add(a[0], b[0]), add(a[1], b[1])))
        odd.append(turn((sub(a[0], b[0]), sub(a[1], b[1])), 2.0 * math.pi * k / size))
    made = [None] * size
    made[0::2] = to_real(even)
    made[1::2] = to_real(odd)
    return made


def fetches(sources, targets, arrivals):
    copies = [
        pltpu.make_async_copy(source, target, arrivals.at[i])
        for i, (source, target) in enumerate(zip(sources, targets))
    ]
    for copy in copies:
        copy.start()
    return copies


def room_for(operands):
    return [pltpu.VMEM(o.shape, o.dtype) for o in operands] + [
        pltpu.SemaphoreType.DMA((len(operands),))
    ]


def pack_kernel(plan, ahead, _, *refs):
    sources, later = refs[:6], refs[6 : 6 + ahead]
    out, carried = refs[6 + ahead], refs[7 + ahead : 7 + 2 * ahead]
    targets, arrivals, others = refs[-8:-2], refs[-2], refs[-1]
    copies = fetches(sources, targets, arrivals)
    later_copies = fetches(later, carried, others)
    charges, kernel, real_table, full_table, kernel_table, turns = targets
    width, block = LANES, plan.block
    copies[0].wait()
    tiles = [
        charges[:, :, a * width : (a + 1) * width].reshape(LANES, width)
        for a in range(plan.radix)
    ]
    spectrum = from_real(tiles)
    copies[2].wait()
    slot, real_at = 0, 0
    for first, modes in plan.groups:
        re, im = spectrum[first]
        size = len(modes) * block
        if im is None:
            columns, table, at = width, real_table, real_at
            real_at += size
            values = re
        else:
            if first == 1:
                copies[3].wait()
                copies[5].wait()
            columns, table, at = 2 * width, full_table, 0
            c, s = turns[first : first + 1, :], turns[plan.radix + first : plan.radix + first + 1, :]
            re, im = re * c - im * s, re * s + im * c
            values = jnp.concatenate([re, im], axis=1)
        high, low = split(values)
        w_high = table[at : at + size, :columns]
        w_low = table[at : at + size, columns:]
        made = dot(
            jnp.concatenate([w_high, w_high, w_low], axis=1),
            jnp.concatenate([high, low, high], axis=1),
            NT,
        )
        for m in range(len(modes)):
            start = (slot + m) * plan.sent
            out[start : start + block, :] = made[m * block : (m + 1) * block]
        slot += len(modes)
    copies[1].wait()
    copies[4].wait()
    made = dot_exact(kernel_table[...], kernel[...].reshape(LANES, plan.count), NT)
    for c in range(2):
        rows = pl.ds(block + c, plan.parts, stride=plan.sent)
        out[rows, :] = made[c * plan.parts : (c + 1) * plan.parts]
    for copy in later_copies:
        copy.wait()


def plane_kernel(plan, shared, arrived, *refs):
    twist, blocks, there, sides, out = refs[:5]
    first_pass, spectra, gains, high_part, low_part, edges = refs[5:]
    nz, ny, parts, reps = plan.nz, plan.ny, plan.parts, plan.replicas
    whole = 2 * LANES

    def apply(size, back):
        high, low = high_part[:size, :], low_part[:size, :]
        values = jnp.concatenate([high, low, high], axis=1)
        high, low = there[:, :whole], there[:, whole:]
        table = jnp.concatenate([high, high, low], axis=1 if back else 0)
        return dot(values, table, NT if back else NN)

    def twisted(re, im, t, sign):
        c = twist[t : t + 1, :]
        s = twist[parts + t : parts + t + 1, :] * sign
        return re * c - im * s, re * s + im * c

    def put(at, size, re, im):
        high, low = split(jnp.concatenate([re, im], axis=1))
        high_part[at : at + size, :] = high
        low_part[at : at + size, :] = low

    for gy in range(ny):
        values = []
        for gz in range(nz):
            at = (gz * ny + gy) * plan.sent
            values.append((arrived[at : at + reps, :], arrived[at + reps : at + 2 * reps, :]))
        for kz, (re, im) in enumerate(transform(values, -1)):
            at = (kz * ny + gy) * 2 * reps
            first_pass[at : at + reps, :] = re
            first_pass[at + reps : at + 2 * reps, :] = im
    lines = jnp.concatenate(
        [arrived[pl.ds(plan.block + c, parts, stride=plan.sent), :] for c in range(2)]
    )
    lines = dot_exact(blocks[...], lines, NN)
    c, s = twist[:parts, :], twist[parts:, :]
    for k in range(2):
        re = lines[2 * k * parts : (2 * k + 1) * parts]
        im = lines[(2 * k + 1) * parts : (2 * k + 2) * parts]
        put(k * parts, parts, re * c - im * s, re * s + im * c)
    made = apply(2 * parts, False)
    plus_re, plus_im = made[:parts, :LANES], made[:parts, LANES:]
    minus_re, minus_im = made[parts:, :LANES], made[parts:, LANES:]
    a_re, a_im = 0.5 * (plus_re + minus_re), 0.5 * (plus_im + minus_im)
    b_re, b_im = 0.5 * (plus_im - minus_im), 0.5 * (minus_re - plus_re)
    is_shared = shared[0] == 0
    scale = 1.0 / (plan.count * plan.count)
    for k, (own, mixed) in enumerate(
        ((plus_re, a_re), (plus_im, a_im), (plus_re, b_re), (plus_im, b_im))
    ):
        gains[k * parts : (k + 1) * parts, :] = jnp.where(is_shared, mixed, own) * scale

    for kz in range(nz):
        values = []
        for gy in range(ny):
            at = (kz * ny + gy) * 2 * reps
            values.append((first_pass[at : at + reps, :], first_pass[at + reps : at + 2 * reps, :]))
        for ky, (re, im) in enumerate(transform(values, -1)):
            t = kz * ny + ky
            put(t * reps, reps, *twisted(re, im, t, 1.0))
    spectra[...] = apply(parts * reps, False)

    for t in range(parts):
        made = []
        for piece in range(2):
            at = t * reps + piece * SUBLANES
            k = 2 * piece * parts + t
            u_re, u_im = gains[k : k + 1, :], gains[parts + k : parts + k + 1, :]
            s_re, s_im = spectra[at : at + SUBLANES, :LANES], spectra[at : at + SUBLANES, LANES:]
            made.append((u_re * s_re - u_im * s_im, u_re * s_im + u_im * s_re))
        put(t * reps, reps, *(jnp.concatenate(pair, axis=0) for pair in zip(*made)))
    spectra[...] = apply(parts * reps, True)

    for kz in range(nz):
        values = []
        for ky in range(ny):
            t = kz * ny + ky
            at = t * reps
            re, im = spectra[at : at + reps, :LANES], spectra[at : at + reps, LANES:]
            values.append(twisted(re, im, t, -1.0))
        for gy, (re, im) in enumerate(transform(values, 1)):
            at = (kz * ny + gy) * 2 * reps
            first_pass[at : at + reps, :] = re
            first_pass[at + reps : at + 2 * reps, :] = im
    for gy in range(ny):
        values = []
        for kz in range(nz):
            at = (kz * ny + gy) * 2 * reps
            values.append((first_pass[at : at + reps, :], first_pass[at + reps : at + 2 * reps, :]))
        for gz, (re, im) in enumerate(transform(values, 1)):
            at = (gz * ny + gy) * plan.back
            out[at : at + reps, :] = re
            out[at + reps : at + 2 * reps, :] = im

    block, rows = plan.block, plan.rows
    lane = lax.broadcasted_iota(jnp.int32, (block, LANES), 1)
    quarter = LANES // 4
    before = lane % rows == rows - 1
    last_plane = lane >= (plan.planes - 1) * rows
    first_planes = lane < 2 * rows
    spare = (lane >= 2 * quarter) & (lane < 3 * quarter)

    def main(gz, gy):
        at = ((gz % nz) * ny + gy % ny) * plan.back
        return out[at : at + block, :]

    def beside(gz, gy):
        at = ((gz % nz) * ny + gy % ny) * block
        return slice(at, at + block)

    for gz in range(nz):
        for gy in range(ny):
            side = jnp.where(before, main(gz, gy - 1), main(gz, gy + 1))
            first_pass[beside(gz, gy), :] = side
            high, low = split(side)
            edges[beside(gz, gy), :LANES] = high
            edges[beside(gz, gy), 2 * LANES : 3 * LANES] = low
    for gz in range(nz):
        for gy in range(ny):
            corner = jnp.where(
                last_plane, first_pass[beside(gz - 1, gy), :], first_pass[beside(gz + 1, gy), :]
            )
            high, low = split(corner)
            edges[beside(gz, gy), LANES : 2 * LANES] = high
            edges[beside(gz, gy), 3 * LANES :] = low
    first_pass[...] = dot(edges[...], jnp.concatenate([sides[...], sides[...]], axis=0), NN)
    for gz in range(nz):
        for gy in range(ny):
            made = jnp.where(first_planes, main(gz + 1, gy), first_pass[beside(gz, gy), :])
            made = jnp.where(last_plane, main(gz - 1, gy), made)
            extra = made[3 * SUBLANES :]
            to = (gz * ny + gy) * plan.back + block
            for piece, start in enumerate((0, quarter, 3 * quarter)):
                value = made[piece * SUBLANES : (piece + 1) * SUBLANES]
                moved = pltpu.roll(extra, (2 * quarter - start) % LANES, 1)
                out[to + piece * SUBLANES : to + (piece + 1) * SUBLANES, :] = jnp.where(
                    spare[:SUBLANES], moved, value
                )


def unpack_kernel(
    plan, steps, arrived, real_table, full_table, stencil, out,
    inside, parts_of, coarse, fine, sent,
):
    reps, block = plan.replicas, plan.block
    wide = 2 * LANES
    lane = lax.broadcasted_iota(jnp.int32, (SUBLANES, LANES), 1)
    quarter = LANES // 4
    slot, real_at, part_at = 0, 0, 0
    found = {}
    for first, modes in plan.groups:
        for m in range(len(modes)):
            at = (slot + m) * plan.back
            inside[m * block : (m + 1) * block, :LANES] = arrived[at : at + block, :]
            packed = [
                arrived[at + block + k * SUBLANES : at + block + (k + 1) * SUBLANES, :]
                for k in range(3)
            ]
            last = jnp.where(
                lane < quarter,
                pltpu.roll(packed[0], 2 * quarter, 1),
                jnp.where(
                    lane < 2 * quarter,
                    pltpu.roll(packed[1], 3 * quarter, 1),
                    pltpu.roll(packed[2], quarter, 1),
                ),
            )
            for k, value in enumerate(packed + [last]):
                to = m * block + k * SUBLANES
                inside[to : to + SUBLANES, LANES:] = value
        depth = len(modes) * block
        high, low = split(inside[:depth, :])
        both = jnp.concatenate([high, low, high], axis=0)
        if first in (0, plan.radix // 2):
            size, table, at = LANES, real_table, real_at
            real_at += size
        else:
            size, table, at = 2 * LANES, full_table, 0
        w_high = table[at : at + size, :depth]
        w_low = table[at : at + size, depth:]
        made = dot(jnp.concatenate([w_high, w_high, w_low], axis=1), both, NN)
        parts_of[part_at : part_at + size, :] = made
        found[first] = (part_at, size > LANES)
        part_at += size
        slot += len(modes)
    for x_l in range(plan.fine_x):
        for piece in range(reps // SUBLANES):
            row = x_l * reps + piece * SUBLANES
            values = []
            for first in range(plan.radix // 2 + 1):
                at, is_full = found[first]
                re = parts_of[at + row : at + row + SUBLANES, :]
                im = None
                if is_full:
                    im = parts_of[at + LANES + row : at + LANES + row + SUBLANES, :]
                value = (re, im)
                if is_full:
                    value = turn(value, 2.0 * math.pi * first * x_l / plan.count)
                values.append(value)
            for xh, value in enumerate(to_real(values)):
                x = xh * plan.fine_x + x_l
                places = [x + 1]
                if x == plan.count - 1:
                    places.append(0)
                if x < 2:
                    places.append(x + 1 + plan.count)
                for place in places:
                    to = place * reps + piece * SUBLANES
                    coarse[to : to + SUBLANES, :] = value

    here = plan.count // steps
    table = jnp.concatenate([stencil[...], stencil[...]], axis=1)
    width = out.shape[2] // steps
    copies = []
    for step in range(steps):
        made = []
        for i in range(here):
            taps = []
            for move in range(4):
                at = (step * here + i + move) * reps
                taps.append(coarse[at : at + reps, :])
            made.append(taps[1])
            made.append((taps[1] + taps[2]) * (9.0 / 16.0) - (taps[0] + taps[3]) * (1.0 / 16.0))
        high, low = split(jnp.concatenate(made, axis=0))
        values = dot(table, jnp.concatenate([high, low], axis=1), NT)
        values = values.reshape(plan.planes + 3, 2 * plan.rows, width)
        for z in range(plan.planes):
            fine[step, 2 * z] = values[z + 1]
            fine[step, 2 * z + 1] = (values[z + 1] + values[z + 2]) * (9.0 / 16.0) - (
                values[z] + values[z + 3]
            ) * (1.0 / 16.0)
        copies.append(
            pltpu.make_async_copy(
                fine.at[step], out.at[:, :, step * width : (step + 1) * width], sent.at[step]
            )
        )
        copies[-1].start()
    for copy in copies:
        copy.wait()


def exchanged(values, parts):
    rows = values.shape[0]
    values = values.reshape(parts, 1, rows // parts * LANES)
    values = lax.all_to_all(values, ("gz", "gy"), split_axis=0, concat_axis=0, tiled=True)
    return values.reshape(rows, LANES)


def in_hbm(arrays):
    return [pltpu.with_memory_space_constraint(array, pltpu.HBM) for array in arrays]


def like(arrays):
    return [jax.ShapeDtypeStruct(array.shape, array.dtype) for array in arrays]


def fast_form(plan, charges, kernel):
    f32, bf16 = jnp.float32, jnp.bfloat16
    parts, reps, block = plan.parts, plan.replicas, plan.block
    limit = pltpu.CompilerParams(vmem_limit_bytes=40 * 1024 * 1024)
    me = (lax.axis_index("gz") * plan.ny + lax.axis_index("gy")).reshape(1)

    operands = [charges, kernel] + [jnp.asarray(t) for t in pack_tables(plan)]
    tables = [jnp.asarray(t) for t in plane_tables(plan)]
    packed, *tables = pl.pallas_call(
        functools.partial(pack_kernel, plan, len(tables)),
        out_shape=[jax.ShapeDtypeStruct((parts * plan.sent, LANES), f32)] + like(tables),
        in_specs=[SMEM] + [HBM] * (len(operands) + len(tables)),
        out_specs=[VMEM] * (1 + len(tables)),
        scratch_shapes=room_for(operands) + [pltpu.SemaphoreType.DMA((len(tables),))],
        compiler_params=limit,
        name="pack",
    )(me, *in_hbm(operands), *in_hbm(tables))
    packed = exchanged(packed, parts)

    later = [jnp.asarray(t) for t in unpack_tables(plan) + (stencil_table(plan),)]
    planes = pl.pallas_call(
        functools.partial(plane_kernel, plan),
        out_shape=jax.ShapeDtypeStruct((parts * plan.back, LANES), f32),
        in_specs=[SMEM] + [VMEM] * (1 + len(tables)),
        out_specs=VMEM,
        scratch_shapes=[
            pltpu.VMEM((parts * block, LANES), f32),
            pltpu.VMEM((parts * reps, 2 * LANES), f32),
            pltpu.VMEM((4 * parts, LANES), f32),
            pltpu.VMEM((parts * reps, 2 * LANES), bf16),
            pltpu.VMEM((parts * reps, 2 * LANES), bf16),
            pltpu.VMEM((parts * block, 4 * LANES), bf16),
        ],
        compiler_params=limit,
        name="plane",
    )(me, packed, *tables)
    planes = exchanged(planes, parts)

    steps = plan.radix
    fine_shape = (2 * plan.planes, 2 * plan.rows, 2 * plan.count * reps)
    return pl.pallas_call(
        functools.partial(unpack_kernel, plan, steps),
        out_shape=jax.ShapeDtypeStruct(fine_shape, f32),
        in_specs=[VMEM] * (1 + len(later)),
        out_specs=HBM,
        scratch_shapes=[
            pltpu.VMEM((2 * LANES, 2 * LANES), f32),
            pltpu.VMEM((plan.radix * LANES, 2 * LANES), f32),
            pltpu.VMEM(((plan.count + 3) * reps, 2 * LANES), f32),
            pltpu.VMEM((steps,) + fine_shape[:2] + (fine_shape[2] // steps,), f32),
            pltpu.SemaphoreType.DMA((steps,)),
        ],
        compiler_params=limit,
        name="unpack",
    )(planes, *later)


def extended(block, sides, width):
    for axis, dim in sides:
        count = lax.axis_size(axis)
        forward_pairs = [(i, (i + 1) % count) for i in range(count)]
        backward_pairs = [(target, source) for source, target in forward_pairs]
        low = lax.ppermute(
            lax.slice_in_dim(block, block.shape[dim] - width, None, axis=dim), axis, forward_pairs
        )
        high = lax.ppermute(lax.slice_in_dim(block, 0, width, axis=dim), axis, backward_pairs)
        block = jnp.concatenate([low, block, high], axis=dim)
    return block


def tables_of(count):
    index = jnp.arange(count, dtype=jnp.int32)
    product = index[:, None] * index[None, :] % count
    angle = product.astype(jnp.float32) * (2.0 * math.pi / count)
    return (jnp.cos(angle), jnp.sin(angle))


def along(values, table, axis):
    moved = jnp.tensordot(values, table, axes=((axis,), (0,)), precision=lax.Precision.HIGHEST)
    return jnp.moveaxis(moved, -1, axis)


def forward(spectrum, axis, cosines, sines):
    real_part, imag_part = (spectrum[0], spectrum[1])
    inner = axis - 1
    new_real = along(real_part, cosines, inner) + along(imag_part, sines, inner)
    new_imag = along(imag_part, cosines, inner) - along(real_part, sines, inner)
    return jnp.stack([new_real, new_imag])


def backward(spectrum, axis, cosines, sines):
    real_part, imag_part = (spectrum[0], spectrum[1])
    inner = axis - 1
    count = cosines.shape[0]
    new_real = (along(real_part, cosines, inner) - along(imag_part, sines, inner)) / count
    new_imag = (along(imag_part, cosines, inner) + along(real_part, sines, inner)) / count
    return jnp.stack([new_real, new_imag])


def refine_rim(haloed, axis, count):
    centre = lax.slice_in_dim(haloed, 2, 2 + count, axis=axis)
    before = lax.slice_in_dim(haloed, 1, 1 + count, axis=axis)
    after = lax.slice_in_dim(haloed, 3, 3 + count, axis=axis)
    after_two = lax.slice_in_dim(haloed, 4, 4 + count, axis=axis)
    middle = (9.0 * (centre + after) - (before + after_two)) / 16.0
    stacked = jnp.stack([centre, middle], axis=axis + 1)
    shape = list(centre.shape)
    shape[axis] = 2 * count
    return stacked.reshape(shape)


def refine_loop(coarse, axis):
    before = jnp.roll(coarse, 1, axis)
    after = jnp.roll(coarse, -1, axis)
    after_two = jnp.roll(coarse, -2, axis)
    middle = (9.0 * (coarse + after) - (before + after_two)) / 16.0
    stacked = jnp.stack([coarse, middle], axis=axis + 1)
    shape = list(coarse.shape)
    shape[axis] = 2 * shape[axis]
    return stacked.reshape(shape)


def general_form(charges, kernel):
    planes, rows, count = (kernel.shape[0], kernel.shape[1], kernel.shape[2])
    replicas = charges.shape[2] // count
    grids = charges.reshape(planes, rows, count, replicas)
    cosines, sines = tables_of(count)
    spectrum = jnp.stack([along(grids, cosines, 2), -along(grids, sines, 2)])
    kernel_spec = jnp.stack([along(kernel, cosines, 2), -along(kernel, sines, 2)])
    spectrum, kernel_spec = (
        lax.all_to_all(spectrum, "gy", split_axis=3, concat_axis=2, tiled=True),
        lax.all_to_all(kernel_spec, "gy", split_axis=3, concat_axis=2, tiled=True),
    )
    spectrum = forward(spectrum, 2, cosines, sines)
    kernel_spec = forward(kernel_spec, 2, cosines, sines)
    spectrum, kernel_spec = (
        lax.all_to_all(spectrum, "gz", split_axis=2, concat_axis=1, tiled=True),
        lax.all_to_all(kernel_spec, "gz", split_axis=2, concat_axis=1, tiled=True),
    )
    spectrum = forward(spectrum, 1, cosines, sines)
    kernel_spec = forward(kernel_spec, 1, cosines, sines)
    kernel_real = kernel_spec[0][..., None]
    kernel_imag = kernel_spec[1][..., None]
    product_real = spectrum[0] * kernel_real - spectrum[1] * kernel_imag
    product_imag = spectrum[1] * kernel_real + spectrum[0] * kernel_imag
    spectrum = backward(jnp.stack([product_real, product_imag]), 1, cosines, sines)
    spectrum = lax.all_to_all(spectrum, "gz", split_axis=1, concat_axis=2, tiled=True)
    spectrum = backward(spectrum, 2, cosines, sines)
    spectrum = lax.all_to_all(spectrum, "gy", split_axis=2, concat_axis=3, tiled=True)
    potential = (along(spectrum[0], cosines, 2) - along(spectrum[1], sines, 2)) / count
    haloed = extended(potential, (("gz", 0), ("gy", 1)), 2)
    result = refine_rim(haloed, 0, planes)
    result = refine_rim(result, 1, rows)
    result = refine_loop(result, 2)
    return result.reshape(2 * planes, 2 * rows, 2 * count * replicas)


def per_device(nz, ny, charges, kernel):
    planes, rows, count = kernel.shape
    replicas = charges.shape[2] // count
    sizes = (planes, rows, count, replicas, nz, ny)
    if Plan.fits(*sizes):
        return fast_form(Plan(*sizes), charges, kernel)
    return general_form(charges, kernel)


def solution(mesh):
    placed = (P("gz", "gy", None), P("gz", "gy", None))
    sizes = (mesh.shape["gz"], mesh.shape["gy"])
    return jax.shard_map(
        functools.partial(per_device, *sizes),
        mesh=mesh,
        in_specs=placed,
        out_specs=P("gz", "gy", None),
        check_vma=False,
    )
```

```python
import functools
import math

import jax
import jax.numpy as jnp
import numpy as np
from jax import lax
from jax.experimental import pallas as pl
from jax.experimental.pallas import tpu as pltpu
from jax.sharding import PartitionSpec as P

LANES = 128
SUBLANES = 8
TAPS = ((-1, -1.0 / 16.0), (0, 9.0 / 16.0), (1, 9.0 / 16.0), (2, -1.0 / 16.0))
VMEM = pl.BlockSpec(memory_space=pltpu.VMEM)
SMEM = pl.BlockSpec(memory_space=pltpu.SMEM)
HBM = pl.BlockSpec(memory_space=pltpu.HBM)
NT = (((1,), (1,)), ((), ()))
NN = (((1,), (0,)), ((), ()))


class Plan:
    def __init__(self, planes, rows, count, replicas, nz, ny):
        self.planes, self.rows, self.count, self.replicas = planes, rows, count, replicas
        self.nz, self.ny = nz, ny
        self.fine_x = LANES // replicas
        self.radix = count // self.fine_x
        self.parts = nz * ny
        self.block = 2 * replicas
        self.sent = self.block + 2
        self.back = self.block + 3 * self.block // 4
        half = self.radix // 2
        groups = [(0, list(range(0, count // 2, self.radix)))]
        groups.append((half, list(range(half, count // 2, self.radix))))
        for first in range(1, half):
            groups.append((first, list(range(first, count, self.radix))))
        self.groups = groups

    @staticmethod
    def fits(planes, rows, count, replicas, nz, ny):
        if planes * rows != LANES or rows % SUBLANES or 2 * rows * 4 != LANES:
            return False
        if LANES % replicas or replicas % SUBLANES or 2 * replicas != 4 * SUBLANES:
            return False
        fine_x = LANES // replicas
        if count % (2 * fine_x):
            return False
        powers = (count // fine_x, nz, ny, fine_x)
        if any(size & (size - 1) for size in powers):
            return False
        return nz * ny * 2 == count and nz > 2 and ny > 2 and count // fine_x >= 4


def halves(table):
    high = np.asarray(table, np.float32).astype(jnp.bfloat16)
    low = (np.asarray(table, np.float64) - high.astype(np.float64)).astype(jnp.bfloat16)
    return high, low


def side_by_side(table):
    return np.concatenate(halves(table), axis=1)


def spread(small, replicas):
    return np.kron(small, np.eye(replicas))


def slot_rows(plan, modes, at, shared=True):
    made = []
    for mode in modes:
        angle = 2.0 * np.pi * mode * at / plan.count
        if shared and mode == 0:
            made.append(np.concatenate([np.cos(angle), np.sin(angle)]))
            flip = np.pi * at
            made.append(np.concatenate([np.cos(flip), np.sin(flip)]))
        else:
            made.append(np.concatenate([np.cos(angle), np.sin(angle)]))
            made.append(np.concatenate([-np.sin(angle), np.cos(angle)]))
    return np.stack(made)


def shared_slot(plan, table):
    half = plan.replicas // 2
    order = [
        (j // half) * plan.replicas + j % half + half * c
        for c in range(2)
        for j in range(plan.replicas)
    ]
    return np.concatenate([table[order], table[plan.block :]])


def full_rows(plan):
    modes = range(0, plan.count, plan.radix)
    return slot_rows(plan, modes, np.arange(plan.fine_x), shared=False)


def pack_tables(plan):
    at = np.arange(plan.fine_x)
    real = []
    for first, modes in plan.groups[:2]:
        table = spread(slot_rows(plan, modes, at)[:, : plan.fine_x], plan.replicas)
        real.append(side_by_side(shared_slot(plan, table) if first == 0 else table))
    turns = np.zeros((2 * plan.radix, LANES))
    for first in range(plan.radix):
        angle = np.repeat(2.0 * np.pi * first * at / plan.count, plan.replicas)
        turns[first], turns[plan.radix + first] = np.cos(angle), -np.sin(angle)
    modes = [mode for _, group in plan.groups for mode in group]
    every = slot_rows(plan, modes, np.arange(plan.count))[:, : plan.count]
    every = np.concatenate([every[0::2], every[1::2]])
    full = side_by_side(spread(full_rows(plan), plan.replicas))
    wide = np.zeros((plan.count, LANES))
    wide[:, : plan.count] = every
    singles = np.concatenate([turns, wide]).astype(np.float32)
    return np.concatenate([full, np.concatenate(real, axis=1)]), singles


def unpack_tables(plan):
    at = np.arange(plan.fine_x)
    real = []
    for first, modes in plan.groups[:2]:
        re_of = slot_rows(plan, modes, at)[:, : plan.fine_x].T
        weight = np.full(re_of.shape, 2.0 / plan.count)
        if first == 0:
            weight[:, :2] = 1.0 / plan.count
        table = spread(re_of * weight, plan.replicas)
        real.append(side_by_side(shared_slot(plan, table.T).T if first == 0 else table))
    full = side_by_side(spread(full_rows(plan).T / plan.count, plan.replicas))
    return np.concatenate(real), full


def plane_tables(plan):
    count = plan.count
    z_at = np.repeat(np.arange(plan.planes), plan.rows)
    y_at = np.tile(np.arange(plan.rows), plan.planes)
    z_of = np.repeat(np.arange(plan.nz), plan.ny)
    y_of = np.tile(np.arange(plan.ny), plan.nz)
    angle = 2 * np.pi * (np.outer(z_of, z_at) + np.outer(y_of, y_at)) / count
    twist = np.concatenate([np.cos(angle), -np.sin(angle)]).astype(np.float32)
    angle = 2 * np.pi * (np.outer(z_at, z_at) / plan.planes + np.outer(y_at, y_at) / plan.rows)
    cosine, sine = np.cos(angle), np.sin(angle)
    there = np.block([[cosine, -sine], [sine, cosine]])
    angle = 2 * np.pi * (np.outer(z_of, z_of) / plan.nz + np.outer(y_of, y_of) / plan.ny)
    cosine, sine = np.cos(angle), np.sin(angle)
    blocks = np.block([[cosine, sine], [-sine, cosine], [cosine, -sine], [-sine, -cosine]])
    wide = np.zeros((blocks.shape[0], LANES), np.float32)
    wide[:, : blocks.shape[1]] = blocks
    doubles = np.concatenate([side_by_side(there), side_table(plan)], axis=1)
    return np.concatenate([twist, wide]), doubles


def halo_places(plan):
    planes, rows = plan.planes, plan.rows
    quarter = LANES // 4
    open_lanes = [
        lane
        for lane in range(2 * rows, (planes - 1) * rows)
        if not 2 * quarter <= lane < 3 * quarter
    ]
    sides = [(z, y) for z in range(-1, planes + 2) for y in (-1, rows, rows + 1)]
    places = dict(zip(sides, open_lanes, strict=False))
    for row in range(rows):
        places[(-1, row)] = (planes - 1) * rows + row
        places[(planes, row)] = row
        places[(planes + 1, row)] = rows + row
    return places


def side_table(plan):
    planes, rows = plan.planes, plan.rows
    table = np.zeros((2 * LANES, LANES))
    for (z, y), lane in halo_places(plan).items():
        if 0 <= y < rows:
            continue
        source = z % planes * rows + y % rows
        table[source if 0 <= z < planes else LANES + source, lane] = 1.0
    return table.astype(jnp.bfloat16)


def stencil_table(plan):
    where = halo_places(plan)

    def line(size):
        made = np.zeros((2 * size, size + 3))
        for i in range(size):
            made[2 * i, i + 1] = 1.0
            for step, weight in TAPS:
                made[2 * i + 1, i + 1 + step] = weight
        return made

    along_z, along_y = np.eye(plan.planes + 3), line(plan.rows)
    table = np.zeros((2 * (plan.planes + 3) * plan.rows, 2 * LANES))
    for z in range(-1, plan.planes + 2):
        for y in range(-1, plan.rows + 2):
            if 0 <= z < plan.planes and 0 <= y < plan.rows:
                lane = z * plan.rows + y
            else:
                lane = LANES + where[(z, y)]
            table[:, lane] = np.kron(along_z[:, z + 1], along_y[:, y + 1])
    return table.astype(jnp.bfloat16)


def split(values):
    high = values.astype(jnp.bfloat16)
    low = (values - high.astype(jnp.float32)).astype(jnp.bfloat16)
    return high, low


def dot(a, b, dims):
    return lax.dot_general(a, b, dims, preferred_element_type=jnp.float32)


def dot_exact(a, b, dims):
    return lax.dot_general(
        a, b, dims, precision=lax.Precision.HIGHEST, preferred_element_type=jnp.float32
    )


def add(a, b):
    if a is None:
        return b
    return a if b is None else a + b


def sub(a, b):
    if b is None:
        return a
    return -b if a is None else a - b


def turn(value, angle):
    re, im = value
    c, s = math.cos(angle), math.sin(angle)
    near = 1e-9
    if abs(s) < near:
        return value if c > 0 else (sub(None, re) if re is not None else None, sub(None, im) if im is not None else None)
    if abs(c) < near:
        minus = lambda v: None if v is None else -v
        return (minus(im), re) if s > 0 else (im, minus(re))
    if abs(abs(c) - abs(s)) < near:
        c_sign, s_sign = math.copysign(1.0, c), math.copysign(1.0, s)
        size = abs(c)
        if im is None:
            scaled = re * size
            return (scaled if c_sign > 0 else -scaled, scaled if s_sign > 0 else -scaled)
        first = (re - im) if c_sign * s_sign > 0 else (re + im)
        second = (re + im) if c_sign * s_sign > 0 else (im - re)
        return (first * (c_sign * size), second * (c_sign * size))
    if im is None:
        return (re * c, re * s)
    return (re * c - im * s, re * s + im * c)


def transform(values, sign):
    size = len(values)
    if size == 1:
        return values
    even, odd = transform(values[0::2], sign), transform(values[1::2], sign)
    first, second = [], []
    for k in range(size // 2):
        e, o = even[k], turn(odd[k], sign * 2.0 * math.pi * k / size)
        first.append((add(e[0], o[0]), add(e[1], o[1])))
        second.append((sub(e[0], o[0]), sub(e[1], o[1])))
    return first + second


def from_real(values):
    size = len(values)
    if size == 2:
        return [(values[0] + values[1], None), (values[0] - values[1], None)]
    even, odd = from_real(values[0::2]), from_real(values[1::2])
    made = [None] * (size // 2 + 1)
    for k in range(size // 4 + 1):
        e, o = even[k], turn(odd[k], -2.0 * math.pi * k / size)
        made[k] = (add(e[0], o[0]), add(e[1], o[1]))
        if size // 2 - k != k:
            other = (sub(e[0], o[0]), sub(e[1], o[1]))
            made[size // 2 - k] = (other[0], None if other[1] is None else -other[1])
    made[0] = (made[0][0], None)
    made[size // 2] = (made[size // 2][0], None)
    return made


def to_real(values):
    half = len(values) - 1
    size = 2 * half
    if size == 2:
        a, b = values[0][0], values[1][0]
        return [a + b, a - b]
    even, odd = [], []
    for k in range(half // 2 + 1):
        a = values[k]
        b = values[half - k]
        b = (b[0], None if b[1] is None else -b[1])
        if k == half // 2:
            even.append((a[0] + b[0], None))
            odd.append((turn((None, sub(a[1], b[1])), 2.0 * math.pi * k / size)[0], None))
            continue
        even.append((add(a[0], b[0]), add(a[1], b[1])))
        odd.append(turn((sub(a[0], b[0]), sub(a[1], b[1])), 2.0 * math.pi * k / size))
    made = [None] * size
    made[0::2] = to_real(even)
    made[1::2] = to_real(odd)
    return made


def fetches(sources, targets, arrivals):
    copies = [
        pltpu.make_async_copy(source, target, arrivals.at[i])
        for i, (source, target) in enumerate(zip(sources, targets))
    ]
    for copy in copies:
        copy.start()
    return copies


def room_for(operands):
    return [pltpu.VMEM(o.shape, o.dtype) for o in operands] + [
        pltpu.SemaphoreType.DMA((len(operands),))
    ]


def pack_kernel(plan, ahead, _, *refs):
    sources, later = refs[:4], refs[4 : 4 + ahead]
    out, carried = refs[4 + ahead], refs[5 + ahead : 5 + 2 * ahead]
    targets, arrivals, others = refs[-6:-2], refs[-2], refs[-1]
    copies = fetches(sources, targets, arrivals)
    later_copies = fetches(later, carried, others)
    charges, kernel, table, singles = targets
    width, block = LANES, plan.block
    copies[0].wait()
    tiles = [
        charges[:, :, a * width : (a + 1) * width].reshape(LANES, width)
        for a in range(plan.radix)
    ]
    spectrum = from_real(tiles)
    copies[2].wait()
    slot, real_at = 0, 0
    for first, modes in plan.groups:
        re, im = spectrum[first]
        size = len(modes) * block
        if im is None:
            rows, at, columns = slice(2 * width, 3 * width), real_at, width
            real_at += 2 * width
            values = re
        else:
            if first == 1:
                copies[3].wait()
            rows, at, columns = slice(0, 2 * width), 0, 2 * width
            c = singles[first : first + 1, :]
            s = singles[plan.radix + first : plan.radix + first + 1, :]
            re, im = re * c - im * s, re * s + im * c
            values = jnp.concatenate([re, im], axis=1)
        high, low = split(values)
        w_high = table[rows, at : at + columns]
        w_low = table[rows, at + columns : at + 2 * columns]
        made = dot(
            jnp.concatenate([w_high, w_high, w_low], axis=1),
            jnp.concatenate([high, low, high], axis=1),
            NT,
        )
        for m in range(len(modes)):
            start = (slot + m) * plan.sent
            out[start : start + block, :] = made[m * block : (m + 1) * block]
        slot += len(modes)
    copies[1].wait()
    made = dot_exact(singles[2 * plan.radix :, : plan.count], kernel[...].reshape(LANES, plan.count), NT)
    for c in range(2):
        rows = pl.ds(block + c, plan.parts, stride=plan.sent)
        out[rows, :] = made[c * plan.parts : (c + 1) * plan.parts]
    for copy in later_copies:
        copy.wait()


def plane_kernel(plan, shared, arrived, *refs):
    twist, there, out = refs[:3]
    first_pass, spectra, gains, high_part, low_part, edges = refs[3:]
    nz, ny, parts, reps = plan.nz, plan.ny, plan.parts, plan.replicas
    whole = 2 * LANES

    def apply(size, back):
        high, low = high_part[:size, :], low_part[:size, :]
        values = jnp.concatenate([high, low, high], axis=1)
        high, low = there[:, :whole], there[:, whole : 2 * whole]
        table = jnp.concatenate([high, high, low], axis=1 if back else 0)
        return dot(values, table, NT if back else NN)

    def twisted(re, im, t, sign):
        c = twist[t : t + 1, :]
        s = twist[parts + t : parts + t + 1, :] * sign
        return re * c - im * s, re * s + im * c

    def put(at, size, re, im):
        high, low = split(jnp.concatenate([re, im], axis=1))
        high_part[at : at + size, :] = high
        low_part[at : at + size, :] = low

    for gy in range(ny):
        values = []
        for gz in range(nz):
            at = (gz * ny + gy) * plan.sent
            values.append((arrived[at : at + reps, :], arrived[at + reps : at + 2 * reps, :]))
        for kz, (re, im) in enumerate(transform(values, -1)):
            at = (kz * ny + gy) * 2 * reps
            first_pass[at : at + reps, :] = re
            first_pass[at + reps : at + 2 * reps, :] = im
    lines = jnp.concatenate(
        [arrived[pl.ds(plan.block + c, parts, stride=plan.sent), :] for c in range(2)]
    )
    lines = dot_exact(twist[2 * parts :, : 2 * parts], lines, NN)
    c, s = twist[:parts, :], twist[parts : 2 * parts, :]
    for k in range(2):
        re = lines[2 * k * parts : (2 * k + 1) * parts]
        im = lines[(2 * k + 1) * parts : (2 * k + 2) * parts]
        put(k * parts, parts, re * c - im * s, re * s + im * c)
    made = apply(2 * parts, False)
    plus_re, plus_im = made[:parts, :LANES], made[:parts, LANES:]
    minus_re, minus_im = made[parts:, :LANES], made[parts:, LANES:]
    a_re, a_im = 0.5 * (plus_re + minus_re), 0.5 * (plus_im + minus_im)
    b_re, b_im = 0.5 * (plus_im - minus_im), 0.5 * (minus_re - plus_re)
    is_shared = shared[0] == 0
    scale = 1.0 / (plan.count * plan.count)
    for k, (own, mixed) in enumerate(
        ((plus_re, a_re), (plus_im, a_im), (plus_re, b_re), (plus_im, b_im))
    ):
        gains[k * parts : (k + 1) * parts, :] = jnp.where(is_shared, mixed, own) * scale

    for kz in range(nz):
        values = []
        for gy in range(ny):
            at = (kz * ny + gy) * 2 * reps
            values.append((first_pass[at : at + reps, :], first_pass[at + reps : at + 2 * reps, :]))
        for ky, (re, im) in enumerate(transform(values, -1)):
            t = kz * ny + ky
            put(t * reps, reps, *twisted(re, im, t, 1.0))
    spectra[...] = apply(parts * reps, False)

    for t in range(parts):
        made = []
        for piece in range(2):
            at = t * reps + piece * SUBLANES
            k = 2 * piece * parts + t
            u_re, u_im = gains[k : k + 1, :], gains[parts + k : parts + k + 1, :]
            s_re, s_im = spectra[at : at + SUBLANES, :LANES], spectra[at : at + SUBLANES, LANES:]
            made.append((u_re * s_re - u_im * s_im, u_re * s_im + u_im * s_re))
        put(t * reps, reps, *(jnp.concatenate(pair, axis=0) for pair in zip(*made)))
    spectra[...] = apply(parts * reps, True)

    for kz in range(nz):
        values = []
        for ky in range(ny):
            t = kz * ny + ky
            at = t * reps
            re, im = spectra[at : at + reps, :LANES], spectra[at : at + reps, LANES:]
            values.append(twisted(re, im, t, -1.0))
        for gy, (re, im) in enumerate(transform(values, 1)):
            at = (kz * ny + gy) * 2 * reps
            first_pass[at : at + reps, :] = re
            first_pass[at + reps : at + 2 * reps, :] = im
    for gy in range(ny):
        values = []
        for kz in range(nz):
            at = (kz * ny + gy) * 2 * reps
            values.append((first_pass[at : at + reps, :], first_pass[at + reps : at + 2 * reps, :]))
        for gz, (re, im) in enumerate(transform(values, 1)):
            at = (gz * ny + gy) * plan.back
            out[at : at + reps, :] = re
            out[at + reps : at + 2 * reps, :] = im

    block, rows = plan.block, plan.rows
    lane = lax.broadcasted_iota(jnp.int32, (block, LANES), 1)
    quarter = LANES // 4
    before = lane % rows == rows - 1
    last_plane = lane >= (plan.planes - 1) * rows
    first_planes = lane < 2 * rows
    spare = (lane >= 2 * quarter) & (lane < 3 * quarter)

    def main(gz, gy):
        at = ((gz % nz) * ny + gy % ny) * plan.back
        return out[at : at + block, :]

    def beside(gz, gy):
        at = ((gz % nz) * ny + gy % ny) * block
        return slice(at, at + block)

    for gz in range(nz):
        for gy in range(ny):
            side = jnp.where(before, main(gz, gy - 1), main(gz, gy + 1))
            first_pass[beside(gz, gy), :] = side
            high, low = split(side)
            edges[beside(gz, gy), :LANES] = high
            edges[beside(gz, gy), 2 * LANES : 3 * LANES] = low
    for gz in range(nz):
        for gy in range(ny):
            corner = jnp.where(
                last_plane, first_pass[beside(gz - 1, gy), :], first_pass[beside(gz + 1, gy), :]
            )
            high, low = split(corner)
            edges[beside(gz, gy), LANES : 2 * LANES] = high
            edges[beside(gz, gy), 3 * LANES :] = low
    first_pass[...] = dot(edges[...], jnp.concatenate([there[:, 2 * whole :]] * 2, axis=0), NN)
    for gz in range(nz):
        for gy in range(ny):
            made = jnp.where(first_planes, main(gz + 1, gy), first_pass[beside(gz, gy), :])
            made = jnp.where(last_plane, main(gz - 1, gy), made)
            extra = made[3 * SUBLANES :]
            to = (gz * ny + gy) * plan.back + block
            for piece, start in enumerate((0, quarter, 3 * quarter)):
                value = made[piece * SUBLANES : (piece + 1) * SUBLANES]
                moved = pltpu.roll(extra, (2 * quarter - start) % LANES, 1)
                out[to + piece * SUBLANES : to + (piece + 1) * SUBLANES, :] = jnp.where(
                    spare[:SUBLANES], moved, value
                )


def unpack_kernel(
    plan, steps, arrived, real_table, full_table, stencil, out,
    inside, parts_of, coarse, fine, sent,
):
    reps, block = plan.replicas, plan.block
    wide = 2 * LANES
    lane = lax.broadcasted_iota(jnp.int32, (SUBLANES, LANES), 1)
    quarter = LANES // 4
    slot, real_at, part_at = 0, 0, 0
    found = {}
    for first, modes in plan.groups:
        for m in range(len(modes)):
            at = (slot + m) * plan.back
            inside[m * block : (m + 1) * block, :LANES] = arrived[at : at + block, :]
            packed = [
                arrived[at + block + k * SUBLANES : at + block + (k + 1) * SUBLANES, :]
                for k in range(3)
            ]
            last = jnp.where(
                lane < quarter,
                pltpu.roll(packed[0], 2 * quarter, 1),
                jnp.where(
                    lane < 2 * quarter,
                    pltpu.roll(packed[1], 3 * quarter, 1),
                    pltpu.roll(packed[2], quarter, 1),
                ),
            )
            for k, value in enumerate(packed + [last]):
                to = m * block + k * SUBLANES
                inside[to : to + SUBLANES, LANES:] = value
        depth = len(modes) * block
        high, low = split(inside[:depth, :])
        both = jnp.concatenate([high, low, high], axis=0)
        if first in (0, plan.radix // 2):
            size, table, at = LANES, real_table, real_at
            real_at += size
        else:
            size, table, at = 2 * LANES, full_table, 0
        w_high = table[at : at + size, :depth]
        w_low = table[at : at + size, depth:]
        made = dot(jnp.concatenate([w_high, w_high, w_low], axis=1), both, NN)
        parts_of[part_at : part_at + size, :] = made
        found[first] = (part_at, size > LANES)
        part_at += size
        slot += len(modes)
    for x_l in range(plan.fine_x):
        for piece in range(reps // SUBLANES):
            row = x_l * reps + piece * SUBLANES
            values = []
            for first in range(plan.radix // 2 + 1):
                at, is_full = found[first]
                re = parts_of[at + row : at + row + SUBLANES, :]
                im = None
                if is_full:
                    im = parts_of[at + LANES + row : at + LANES + row + SUBLANES, :]
                value = (re, im)
                if is_full:
                    value = turn(value, 2.0 * math.pi * first * x_l / plan.count)
                values.append(value)
            for xh, value in enumerate(to_real(values)):
                x = xh * plan.fine_x + x_l
                places = [x + 1]
                if x == plan.count - 1:
                    places.append(0)
                if x < 2:
                    places.append(x + 1 + plan.count)
                for place in places:
                    to = place * reps + piece * SUBLANES
                    coarse[to : to + SUBLANES, :] = value

    here = plan.count // steps
    table = jnp.concatenate([stencil[...], stencil[...]], axis=1)
    width = out.shape[2] // steps
    copies = []
    for step in range(steps):
        made = []
        for i in range(here):
            taps = []
            for move in range(4):
                at = (step * here + i + move) * reps
                taps.append(coarse[at : at + reps, :])
            made.append(taps[1])
            made.append((taps[1] + taps[2]) * (9.0 / 16.0) - (taps[0] + taps[3]) * (1.0 / 16.0))
        high, low = split(jnp.concatenate(made, axis=0))
        values = dot(table, jnp.concatenate([high, low], axis=1), NT)
        values = values.reshape(plan.planes + 3, 2 * plan.rows, width)
        for z in range(plan.planes):
            fine[step, 2 * z] = values[z + 1]
            fine[step, 2 * z + 1] = (values[z + 1] + values[z + 2]) * (9.0 / 16.0) - (
                values[z] + values[z + 3]
            ) * (1.0 / 16.0)
        copies.append(
            pltpu.make_async_copy(
                fine.at[step], out.at[:, :, step * width : (step + 1) * width], sent.at[step]
            )
        )
        copies[-1].start()
    for copy in copies:
        copy.wait()


def exchanged(values, parts):
    rows = values.shape[0]
    values = values.reshape(parts, 1, rows // parts * LANES)
    values = lax.all_to_all(values, ("gz", "gy"), split_axis=0, concat_axis=0, tiled=True)
    return values.reshape(rows, LANES)


def in_hbm(arrays):
    return [pltpu.with_memory_space_constraint(array, pltpu.HBM) for array in arrays]


def like(arrays):
    return [jax.ShapeDtypeStruct(array.shape, array.dtype) for array in arrays]


def fast_form(plan, charges, kernel):
    f32, bf16 = jnp.float32, jnp.bfloat16
    parts, reps, block = plan.parts, plan.replicas, plan.block
    limit = pltpu.CompilerParams(vmem_limit_bytes=40 * 1024 * 1024)
    me = (lax.axis_index("gz") * plan.ny + lax.axis_index("gy")).reshape(1)

    operands = [charges, kernel] + [jnp.asarray(t) for t in pack_tables(plan)]
    tables = [jnp.asarray(t) for t in plane_tables(plan)]
    packed, *tables = pl.pallas_call(
        functools.partial(pack_kernel, plan, len(tables)),
        out_shape=[jax.ShapeDtypeStruct((parts * plan.sent, LANES), f32)] + like(tables),
        in_specs=[SMEM] + [HBM] * (len(operands) + len(tables)),
        out_specs=[VMEM] * (1 + len(tables)),
        scratch_shapes=room_for(operands) + [pltpu.SemaphoreType.DMA((len(tables),))],
        compiler_params=limit,
        name="pack",
    )(me, *in_hbm(operands), *in_hbm(tables))
    packed = exchanged(packed, parts)

    later = [jnp.asarray(t) for t in unpack_tables(plan) + (stencil_table(plan),)]
    planes = pl.pallas_call(
        functools.partial(plane_kernel, plan),
        out_shape=jax.ShapeDtypeStruct((parts * plan.back, LANES), f32),
        in_specs=[SMEM] + [VMEM] * (1 + len(tables)),
        out_specs=VMEM,
        scratch_shapes=[
            pltpu.VMEM((parts * block, LANES), f32),
            pltpu.VMEM((parts * reps, 2 * LANES), f32),
            pltpu.VMEM((4 * parts, LANES), f32),
            pltpu.VMEM((parts * reps, 2 * LANES), bf16),
            pltpu.VMEM((parts * reps, 2 * LANES), bf16),
            pltpu.VMEM((parts * block, 4 * LANES), bf16),
        ],
        compiler_params=limit,
        name="plane",
    )(me, packed, *tables)
    planes = exchanged(planes, parts)

    steps = plan.radix
    fine_shape = (2 * plan.planes, 2 * plan.rows, 2 * plan.count * reps)
    return pl.pallas_call(
        functools.partial(unpack_kernel, plan, steps),
        out_shape=jax.ShapeDtypeStruct(fine_shape, f32),
        in_specs=[VMEM] * (1 + len(later)),
        out_specs=HBM,
        scratch_shapes=[
            pltpu.VMEM((2 * LANES, 2 * LANES), f32),
            pltpu.VMEM((plan.radix * LANES, 2 * LANES), f32),
            pltpu.VMEM(((plan.count + 3) * reps, 2 * LANES), f32),
            pltpu.VMEM((steps,) + fine_shape[:2] + (fine_shape[2] // steps,), f32),
            pltpu.SemaphoreType.DMA((steps,)),
        ],
        compiler_params=limit,
        name="unpack",
    )(planes, *later)


def extended(block, sides, width):
    for axis, dim in sides:
        count = lax.axis_size(axis)
        forward_pairs = [(i, (i + 1) % count) for i in range(count)]
        backward_pairs = [(target, source) for source, target in forward_pairs]
        low = lax.ppermute(
            lax.slice_in_dim(block, block.shape[dim] - width, None, axis=dim), axis, forward_pairs
        )
        high = lax.ppermute(lax.slice_in_dim(block, 0, width, axis=dim), axis, backward_pairs)
        block = jnp.concatenate([low, block, high], axis=dim)
    return block


def tables_of(count):
    index = jnp.arange(count, dtype=jnp.int32)
    product = index[:, None] * index[None, :] % count
    angle = product.astype(jnp.float32) * (2.0 * math.pi / count)
    return (jnp.cos(angle), jnp.sin(angle))


def along(values, table, axis):
    moved = jnp.tensordot(values, table, axes=((axis,), (0,)), precision=lax.Precision.HIGHEST)
    return jnp.moveaxis(moved, -1, axis)


def forward(spectrum, axis, cosines, sines):
    real_part, imag_part = (spectrum[0], spectrum[1])
    inner = axis - 1
    new_real = along(real_part, cosines, inner) + along(imag_part, sines, inner)
    new_imag = along(imag_part, cosines, inner) - along(real_part, sines, inner)
    return jnp.stack([new_real, new_imag])


def backward(spectrum, axis, cosines, sines):
    real_part, imag_part = (spectrum[0], spectrum[1])
    inner = axis - 1
    count = cosines.shape[0]
    new_real = (along(real_part, cosines, inner) - along(imag_part, sines, inner)) / count
    new_imag = (along(imag_part, cosines, inner) + along(real_part, sines, inner)) / count
    return jnp.stack([new_real, new_imag])


def refine_rim(haloed, axis, count):
    centre = lax.slice_in_dim(haloed, 2, 2 + count, axis=axis)
    before = lax.slice_in_dim(haloed, 1, 1 + count, axis=axis)
    after = lax.slice_in_dim(haloed, 3, 3 + count, axis=axis)
    after_two = lax.slice_in_dim(haloed, 4, 4 + count, axis=axis)
    middle = (9.0 * (centre + after) - (before + after_two)) / 16.0
    stacked = jnp.stack([centre, middle], axis=axis + 1)
    shape = list(centre.shape)
    shape[axis] = 2 * count
    return stacked.reshape(shape)


def refine_loop(coarse, axis):
    before = jnp.roll(coarse, 1, axis)
    after = jnp.roll(coarse, -1, axis)
    after_two = jnp.roll(coarse, -2, axis)
    middle = (9.0 * (coarse + after) - (before + after_two)) / 16.0
    stacked = jnp.stack([coarse, middle], axis=axis + 1)
    shape = list(coarse.shape)
    shape[axis] = 2 * shape[axis]
    return stacked.reshape(shape)


def general_form(charges, kernel):
    planes, rows, count = (kernel.shape[0], kernel.shape[1], kernel.shape[2])
    replicas = charges.shape[2] // count
    grids = charges.reshape(planes, rows, count, replicas)
    cosines, sines = tables_of(count)
    spectrum = jnp.stack([along(grids, cosines, 2), -along(grids, sines, 2)])
    kernel_spec = jnp.stack([along(kernel, cosines, 2), -along(kernel, sines, 2)])
    spectrum, kernel_spec = (
        lax.all_to_all(spectrum, "gy", split_axis=3, concat_axis=2, tiled=True),
        lax.all_to_all(kernel_spec, "gy", split_axis=3, concat_axis=2, tiled=True),
    )
    spectrum = forward(spectrum, 2, cosines, sines)
    kernel_spec = forward(kernel_spec, 2, cosines, sines)
    spectrum, kernel_spec = (
        lax.all_to_all(spectrum, "gz", split_axis=2, concat_axis=1, tiled=True),
        lax.all_to_all(kernel_spec, "gz", split_axis=2, concat_axis=1, tiled=True),
    )
    spectrum = forward(spectrum, 1, cosines, sines)
    kernel_spec = forward(kernel_spec, 1, cosines, sines)
    kernel_real = kernel_spec[0][..., None]
    kernel_imag = kernel_spec[1][..., None]
    product_real = spectrum[0] * kernel_real - spectrum[1] * kernel_imag
    product_imag = spectrum[1] * kernel_real + spectrum[0] * kernel_imag
    spectrum = backward(jnp.stack([product_real, product_imag]), 1, cosines, sines)
    spectrum = lax.all_to_all(spectrum, "gz", split_axis=1, concat_axis=2, tiled=True)
    spectrum = backward(spectrum, 2, cosines, sines)
    spectrum = lax.all_to_all(spectrum, "gy", split_axis=2, concat_axis=3, tiled=True)
    potential = (along(spectrum[0], cosines, 2) - along(spectrum[1], sines, 2)) / count
    haloed = extended(potential, (("gz", 0), ("gy", 1)), 2)
    result = refine_rim(haloed, 0, planes)
    result = refine_rim(result, 1, rows)
    result = refine_loop(result, 2)
    return result.reshape(2 * planes, 2 * rows, 2 * count * replicas)


def per_device(nz, ny, charges, kernel):
    planes, rows, count = kernel.shape
    replicas = charges.shape[2] // count
    sizes = (planes, rows, count, replicas, nz, ny)
    if Plan.fits(*sizes):
        return fast_form(Plan(*sizes), charges, kernel)
    return general_form(charges, kernel)


def solution(mesh):
    placed = (P("gz", "gy", None), P("gz", "gy", None))
    sizes = (mesh.shape["gz"], mesh.shape["gy"])
    return jax.shard_map(
        functools.partial(per_device, *sizes),
        mesh=mesh,
        in_specs=placed,
        out_specs=P("gz", "gy", None),
        check_vma=False,
    )
```

```python
import functools
import math

import jax
import jax.numpy as jnp
import numpy as np
from jax import lax
from jax.experimental import pallas as pl
from jax.experimental.pallas import tpu as pltpu
from jax.sharding import PartitionSpec as P

LANES = 128
SUBLANES = 8
TAPS = ((-1, -1.0 / 16.0), (0, 9.0 / 16.0), (1, 9.0 / 16.0), (2, -1.0 / 16.0))
VMEM = pl.BlockSpec(memory_space=pltpu.VMEM)
SMEM = pl.BlockSpec(memory_space=pltpu.SMEM)
HBM = pl.BlockSpec(memory_space=pltpu.HBM)
NT = (((1,), (1,)), ((), ()))
NN = (((1,), (0,)), ((), ()))


class Plan:
    def __init__(self, planes, rows, count, replicas, nz, ny):
        self.planes, self.rows, self.count, self.replicas = planes, rows, count, replicas
        self.nz, self.ny = nz, ny
        self.fine_x = LANES // replicas
        self.radix = count // self.fine_x
        self.parts = nz * ny
        self.block = 2 * replicas
        self.sent = self.block + 2
        self.back = self.block + 3 * self.block // 4
        half = self.radix // 2
        groups = [(0, list(range(0, count // 2, self.radix)))]
        groups.append((half, list(range(half, count // 2, self.radix))))
        for first in range(1, half):
            groups.append((first, list(range(first, count, self.radix))))
        self.groups = groups

    @staticmethod
    def fits(planes, rows, count, replicas, nz, ny):
        if planes * rows != LANES or rows % SUBLANES or 2 * rows * 4 != LANES:
            return False
        if LANES % replicas or replicas % SUBLANES or 2 * replicas != 4 * SUBLANES:
            return False
        fine_x = LANES // replicas
        if count % (2 * fine_x):
            return False
        powers = (count // fine_x, nz, ny, fine_x)
        if any(size & (size - 1) for size in powers):
            return False
        return nz * ny * 2 == count and nz > 2 and ny > 2 and count // fine_x >= 4


def halves(table):
    high = np.asarray(table, np.float32).astype(jnp.bfloat16)
    low = (np.asarray(table, np.float64) - high.astype(np.float64)).astype(jnp.bfloat16)
    return high, low


def side_by_side(table):
    return np.concatenate(halves(table), axis=1)


def spread(small, replicas):
    return np.kron(small, np.eye(replicas))


def slot_rows(plan, modes, at, shared=True):
    made = []
    for mode in modes:
        angle = 2.0 * np.pi * mode * at / plan.count
        if shared and mode == 0:
            made.append(np.concatenate([np.cos(angle), np.sin(angle)]))
            flip = np.pi * at
            made.append(np.concatenate([np.cos(flip), np.sin(flip)]))
        else:
            made.append(np.concatenate([np.cos(angle), np.sin(angle)]))
            made.append(np.concatenate([-np.sin(angle), np.cos(angle)]))
    return np.stack(made)


def shared_slot(plan, table):
    half = plan.replicas // 2
    order = [
        (j // half) * plan.replicas + j % half + half * c
        for c in range(2)
        for j in range(plan.replicas)
    ]
    return np.concatenate([table[order], table[plan.block :]])


def full_rows(plan):
    modes = range(0, plan.count, plan.radix)
    return slot_rows(plan, modes, np.arange(plan.fine_x), shared=False)


def pack_tables(plan):
    at = np.arange(plan.fine_x)
    real = []
    for first, modes in plan.groups[:2]:
        table = spread(slot_rows(plan, modes, at)[:, : plan.fine_x], plan.replicas)
        real.append(side_by_side(shared_slot(plan, table) if first == 0 else table))
    turns = np.zeros((2 * plan.radix, LANES))
    for first in range(plan.radix):
        angle = np.repeat(2.0 * np.pi * first * at / plan.count, plan.replicas)
        turns[first], turns[plan.radix + first] = np.cos(angle), -np.sin(angle)
    modes = [mode for _, group in plan.groups for mode in group]
    every = slot_rows(plan, modes, np.arange(plan.count))[:, : plan.count]
    every = np.concatenate([every[0::2], every[1::2]])
    full = side_by_side(spread(full_rows(plan), plan.replicas))
    single = np.float32
    return np.concatenate(real), full, every.astype(single), turns.astype(single)


def unpack_tables(plan):
    at = np.arange(plan.fine_x)
    real = []
    for first, modes in plan.groups[:2]:
        re_of = slot_rows(plan, modes, at)[:, : plan.fine_x].T
        weight = np.full(re_of.shape, 2.0 / plan.count)
        if first == 0:
            weight[:, :2] = 1.0 / plan.count
        table = spread(re_of * weight, plan.replicas)
        real.append(side_by_side(shared_slot(plan, table.T).T if first == 0 else table))
    full = side_by_side(spread(full_rows(plan).T / plan.count, plan.replicas))
    return np.concatenate(real), full


def plane_tables(plan):
    count = plan.count
    z_at = np.repeat(np.arange(plan.planes), plan.rows)
    y_at = np.tile(np.arange(plan.rows), plan.planes)
    z_of = np.repeat(np.arange(plan.nz), plan.ny)
    y_of = np.tile(np.arange(plan.ny), plan.nz)
    angle = 2 * np.pi * (np.outer(z_of, z_at) + np.outer(y_of, y_at)) / count
    twist = np.concatenate([np.cos(angle), -np.sin(angle)]).astype(np.float32)
    angle = 2 * np.pi * (np.outer(z_at, z_at) / plan.planes + np.outer(y_at, y_at) / plan.rows)
    cosine, sine = np.cos(angle), np.sin(angle)
    there = np.block([[cosine, -sine], [sine, cosine]])
    angle = 2 * np.pi * (np.outer(z_of, z_of) / plan.nz + np.outer(y_of, y_of) / plan.ny)
    cosine, sine = np.cos(angle), np.sin(angle)
    blocks = np.block([[cosine, sine], [-sine, cosine], [cosine, -sine], [-sine, -cosine]])
    return twist, blocks.astype(np.float32), side_by_side(there), side_table(plan)


def halo_places(plan):
    planes, rows = plan.planes, plan.rows
    quarter = LANES // 4
    open_lanes = [
        lane
        for lane in range(2 * rows, (planes - 1) * rows)
        if not 2 * quarter <= lane < 3 * quarter
    ]
    sides = [(z, y) for z in range(-1, planes + 2) for y in (-1, rows, rows + 1)]
    places = dict(zip(sides, open_lanes, strict=False))
    for row in range(rows):
        places[(-1, row)] = (planes - 1) * rows + row
        places[(planes, row)] = row
        places[(planes + 1, row)] = rows + row
    return places


def side_table(plan):
    planes, rows = plan.planes, plan.rows
    table = np.zeros((2 * LANES, LANES))
    for (z, y), lane in halo_places(plan).items():
        if 0 <= y < rows:
            continue
        source = z % planes * rows + y % rows
        table[source if 0 <= z < planes else LANES + source, lane] = 1.0
    return table.astype(jnp.bfloat16)


def stencil_table(plan):
    where = halo_places(plan)

    def line(size):
        made = np.zeros((2 * size, size + 3))
        for i in range(size):
            made[2 * i, i + 1] = 1.0
            for step, weight in TAPS:
                made[2 * i + 1, i + 1 + step] = weight
        return made

    along_z, along_y = np.eye(plan.planes + 3), line(plan.rows)
    table = np.zeros((2 * (plan.planes + 3) * plan.rows, 2 * LANES))
    for z in range(-1, plan.planes + 2):
        for y in range(-1, plan.rows + 2):
            if 0 <= z < plan.planes and 0 <= y < plan.rows:
                lane = z * plan.rows + y
            else:
                lane = LANES + where[(z, y)]
            table[:, lane] = np.kron(along_z[:, z + 1], along_y[:, y + 1])
    return table.astype(jnp.bfloat16)


def split(values):
    high = values.astype(jnp.bfloat16)
    low = (values - high.astype(jnp.float32)).astype(jnp.bfloat16)
    return high, low


def dot(a, b, dims):
    return lax.dot_general(a, b, dims, preferred_element_type=jnp.float32)


def dot_exact(a, b, dims):
    return lax.dot_general(
        a, b, dims, precision=lax.Precision.HIGHEST, preferred_element_type=jnp.float32
    )


def add(a, b):
    if a is None:
        return b
    return a if b is None else a + b


def sub(a, b):
    if b is None:
        return a
    return -b if a is None else a - b


def turn(value, angle):
    re, im = value
    c, s = math.cos(angle), math.sin(angle)
    near = 1e-9
    if abs(s) < near:
        return value if c > 0 else (sub(None, re) if re is not None else None, sub(None, im) if im is not None else None)
    if abs(c) < near:
        minus = lambda v: None if v is None else -v
        return (minus(im), re) if s > 0 else (im, minus(re))
    if abs(abs(c) - abs(s)) < near:
        c_sign, s_sign = math.copysign(1.0, c), math.copysign(1.0, s)
        size = abs(c)
        if im is None:
            scaled = re * size
            return (scaled if c_sign > 0 else -scaled, scaled if s_sign > 0 else -scaled)
        first = (re - im) if c_sign * s_sign > 0 else (re + im)
        second = (re + im) if c_sign * s_sign > 0 else (im - re)
        return (first * (c_sign * size), second * (c_sign * size))
    if im is None:
        return (re * c, re * s)
    return (re * c - im * s, re * s + im * c)


def transform(values, sign):
    size = len(values)
    if size == 1:
        return values
    even, odd = transform(values[0::2], sign), transform(values[1::2], sign)
    first, second = [], []
    for k in range(size // 2):
        e, o = even[k], turn(odd[k], sign * 2.0 * math.pi * k / size)
        first.append((add(e[0], o[0]), add(e[1], o[1])))
        second.append((sub(e[0], o[0]), sub(e[1], o[1])))
    return first + second


def from_real(values):
    size = len(values)
    if size == 2:
        return [(values[0] + values[1], None), (values[0] - values[1], None)]
    even, odd = from_real(values[0::2]), from_real(values[1::2])
    made = [None] * (size // 2 + 1)
    for k in range(size // 4 + 1):
        e, o = even[k], turn(odd[k], -2.0 * math.pi * k / size)
        made[k] = (add(e[0], o[0]), add(e[1], o[1]))
        if size // 2 - k != k:
            other = (sub(e[0], o[0]), sub(e[1], o[1]))
            made[size // 2 - k] = (other[0], None if other[1] is None else -other[1])
    made[0] = (made[0][0], None)
    made[size // 2] = (made[size // 2][0], None)
    return made


def to_real(values):
    half = len(values) - 1
    size = 2 * half
    if size == 2:
        a, b = values[0][0], values[1][0]
        return [a + b, a - b]
    even, odd = [], []
    for k in range(half // 2 + 1):
        a = values[k]
        b = values[half - k]
        b = (b[0], None if b[1] is None else -b[1])
        if k == half // 2:
            even.append((a[0] + b[0], None))
            odd.append((turn((None, sub(a[1], b[1])), 2.0 * math.pi * k / size)[0], None))
            continue
        even.append((add(a[0], b[0]), add(a[1], b[1])))
        odd.append(turn((sub(a[0], b[0]), sub(a[1], b[1])), 2.0 * math.pi * k / size))
    made = [None] * size
    made[0::2] = to_real(even)
    made[1::2] = to_real(odd)
    return made


def fetches(sources, targets, arrivals):
    copies = [
        pltpu.make_async_copy(source, target, arrivals.at[i])
        for i, (source, target) in enumerate(zip(sources, targets))
    ]
    for copy in copies:
        copy.start()
    return copies


def room_for(operands):
    return [pltpu.VMEM(o.shape, o.dtype) for o in operands] + [
        pltpu.SemaphoreType.DMA((len(operands),))
    ]


def pack_kernel(plan, ahead, _, *refs):
    sources, later = refs[:6], refs[6 : 6 + ahead]
    out, carried = refs[6 + ahead], refs[7 + ahead : 7 + 2 * ahead]
    targets, arrivals, others = refs[-8:-2], refs[-2], refs[-1]
    copies = fetches(sources, targets, arrivals)
    later_copies = fetches(later, carried, others)
    charges, kernel, real_table, full_table, kernel_table, turns = targets
    width, block = LANES, plan.block
    copies[0].wait()
    tiles = [
        charges[:, :, a * width : (a + 1) * width].reshape(LANES, width)
        for a in range(plan.radix)
    ]
    spectrum = from_real(tiles)
    copies[2].wait()
    slot, real_at = 0, 0
    for first, modes in plan.groups:
        re, im = spectrum[first]
        size = len(modes) * block
        if im is None:
            columns, table, at = width, real_table, real_at
            real_at += size
            values = re
        else:
            if first == 1:
                copies[3].wait()
                copies[5].wait()
            columns, table, at = 2 * width, full_table, 0
            c, s = turns[first : first + 1, :], turns[plan.radix + first : plan.radix + first + 1, :]
            re, im = re * c - im * s, re * s + im * c
            values = jnp.concatenate([re, im], axis=1)
        high, low = split(values)
        w_high = table[at : at + size, :columns]
        w_low = table[at : at + size, columns:]
        made = dot(
            jnp.concatenate([w_high, w_high, w_low], axis=1),
            jnp.concatenate([high, low, high], axis=1),
            NT,
        )
        for m in range(len(modes)):
            start = (slot + m) * plan.sent
            out[start : start + block, :] = made[m * block : (m + 1) * block]
        slot += len(modes)
    copies[1].wait()
    copies[4].wait()
    made = dot_exact(kernel_table[...], kernel[...].reshape(LANES, plan.count), NT)
    for c in range(2):
        rows = pl.ds(block + c, plan.parts, stride=plan.sent)
        out[rows, :] = made[c * plan.parts : (c + 1) * plan.parts]
    for copy in later_copies:
        copy.wait()


def plane_kernel(plan, shared, arrived, *refs):
    twist, blocks, there, sides, out = refs[:5]
    first_pass, spectra, gains, high_part, low_part, edges = refs[5:]
    nz, ny, parts, reps = plan.nz, plan.ny, plan.parts, plan.replicas
    whole = 2 * LANES

    def apply(size, back):
        high, low = high_part[:size, :], low_part[:size, :]
        values = jnp.concatenate([high, low, high], axis=1)
        high, low = there[:, :whole], there[:, whole:]
        table = jnp.concatenate([high, high, low], axis=1 if back else 0)
        return dot(values, table, NT if back else NN)

    def twisted(re, im, t, sign):
        c = twist[t : t + 1, :]
        s = twist[parts + t : parts + t + 1, :] * sign
        return re * c - im * s, re * s + im * c

    def put(at, size, re, im):
        high, low = split(jnp.concatenate([re, im], axis=1))
        high_part[at : at + size, :] = high
        low_part[at : at + size, :] = low

    for gy in range(ny):
        values = []
        for gz in range(nz):
            at = (gz * ny + gy) * plan.sent
            values.append((arrived[at : at + reps, :], arrived[at + reps : at + 2 * reps, :]))
        for kz, (re, im) in enumerate(transform(values, -1)):
            at = (kz * ny + gy) * 2 * reps
            first_pass[at : at + reps, :] = re
            first_pass[at + reps : at + 2 * reps, :] = im
    lines = jnp.concatenate(
        [arrived[pl.ds(plan.block + c, parts, stride=plan.sent), :] for c in range(2)]
    )
    lines = dot_exact(blocks[...], lines, NN)
    c, s = twist[:parts, :], twist[parts:, :]
    for k in range(2):
        re = lines[2 * k * parts : (2 * k + 1) * parts]
        im = lines[(2 * k + 1) * parts : (2 * k + 2) * parts]
        put(k * parts, parts, re * c - im * s, re * s + im * c)
    made = apply(2 * parts, False)
    plus_re, plus_im = made[:parts, :LANES], made[:parts, LANES:]
    minus_re, minus_im = made[parts:, :LANES], made[parts:, LANES:]
    a_re, a_im = 0.5 * (plus_re + minus_re), 0.5 * (plus_im + minus_im)
    b_re, b_im = 0.5 * (plus_im - minus_im), 0.5 * (minus_re - plus_re)
    is_shared = shared[0] == 0
    scale = 1.0 / (plan.count * plan.count)
    for k, (own, mixed) in enumerate(
        ((plus_re, a_re), (plus_im, a_im), (plus_re, b_re), (plus_im, b_im))
    ):
        gains[k * parts : (k + 1) * parts, :] = jnp.where(is_shared, mixed, own) * scale

    for kz in range(nz):
        values = []
        for gy in range(ny):
            at = (kz * ny + gy) * 2 * reps
            values.append((first_pass[at : at + reps, :], first_pass[at + reps : at + 2 * reps, :]))
        for ky, (re, im) in enumerate(transform(values, -1)):
            t = kz * ny + ky
            put(t * reps, reps, *twisted(re, im, t, 1.0))
    spectra[...] = apply(parts * reps, False)

    for t in range(parts):
        made = []
        for piece in range(2):
            at = t * reps + piece * SUBLANES
            k = 2 * piece * parts + t
            u_re, u_im = gains[k : k + 1, :], gains[parts + k : parts + k + 1, :]
            s_re, s_im = spectra[at : at + SUBLANES, :LANES], spectra[at : at + SUBLANES, LANES:]
            made.append((u_re * s_re - u_im * s_im, u_re * s_im + u_im * s_re))
        put(t * reps, reps, *(jnp.concatenate(pair, axis=0) for pair in zip(*made)))
    spectra[...] = apply(parts * reps, True)

    for kz in range(nz):
        values = []
        for ky in range(ny):
            t = kz * ny + ky
            at = t * reps
            re, im = spectra[at : at + reps, :LANES], spectra[at : at + reps, LANES:]
            values.append(twisted(re, im, t, -1.0))
        for gy, (re, im) in enumerate(transform(values, 1)):
            at = (kz * ny + gy) * 2 * reps
            first_pass[at : at + reps, :] = re
            first_pass[at + reps : at + 2 * reps, :] = im
    for gy in range(ny):
        values = []
        for kz in range(nz):
            at = (kz * ny + gy) * 2 * reps
            values.append((first_pass[at : at + reps, :], first_pass[at + reps : at + 2 * reps, :]))
        for gz, (re, im) in enumerate(transform(values, 1)):
            at = (gz * ny + gy) * plan.back
            out[at : at + reps, :] = re
            out[at + reps : at + 2 * reps, :] = im

    block, rows = plan.block, plan.rows
    lane = lax.broadcasted_iota(jnp.int32, (block, LANES), 1)
    quarter = LANES // 4
    before = lane % rows == rows - 1
    last_plane = lane >= (plan.planes - 1) * rows
    first_planes = lane < 2 * rows
    spare = (lane >= 2 * quarter) & (lane < 3 * quarter)

    def main(gz, gy):
        at = ((gz % nz) * ny + gy % ny) * plan.back
        return out[at : at + block, :]

    def beside(gz, gy):
        at = ((gz % nz) * ny + gy % ny) * block
        return slice(at, at + block)

    for gz in range(nz):
        for gy in range(ny):
            side = jnp.where(before, main(gz, gy - 1), main(gz, gy + 1))
            first_pass[beside(gz, gy), :] = side
            high, low = split(side)
            edges[beside(gz, gy), :LANES] = high
            edges[beside(gz, gy), 2 * LANES : 3 * LANES] = low
    for gz in range(nz):
        for gy in range(ny):
            corner = jnp.where(
                last_plane, first_pass[beside(gz - 1, gy), :], first_pass[beside(gz + 1, gy), :]
            )
            high, low = split(corner)
            edges[beside(gz, gy), LANES : 2 * LANES] = high
            edges[beside(gz, gy), 3 * LANES :] = low
    first_pass[...] = dot(edges[...], jnp.concatenate([sides[...], sides[...]], axis=0), NN)
    for gz in range(nz):
        for gy in range(ny):
            made = jnp.where(first_planes, main(gz + 1, gy), first_pass[beside(gz, gy), :])
            made = jnp.where(last_plane, main(gz - 1, gy), made)
            extra = made[3 * SUBLANES :]
            to = (gz * ny + gy) * plan.back + block
            for piece, start in enumerate((0, quarter, 3 * quarter)):
                value = made[piece * SUBLANES : (piece + 1) * SUBLANES]
                moved = pltpu.roll(extra, (2 * quarter - start) % LANES, 1)
                out[to + piece * SUBLANES : to + (piece + 1) * SUBLANES, :] = jnp.where(
                    spare[:SUBLANES], moved, value
                )


def unpack_kernel(
    plan, steps, arrived, real_table, full_table, stencil, out,
    inside, parts_of, coarse, fine, sent,
):
    reps, block = plan.replicas, plan.block
    wide = 2 * LANES
    lane = lax.broadcasted_iota(jnp.int32, (SUBLANES, LANES), 1)
    quarter = LANES // 4
    slot, real_at, part_at = 0, 0, 0
    found = {}
    for first, modes in plan.groups:
        for m in range(len(modes)):
            at = (slot + m) * plan.back
            inside[m * block : (m + 1) * block, :LANES] = arrived[at : at + block, :]
            packed = [
                arrived[at + block + k * SUBLANES : at + block + (k + 1) * SUBLANES, :]
                for k in range(3)
            ]
            last = jnp.where(
                lane < quarter,
                pltpu.roll(packed[0], 2 * quarter, 1),
                jnp.where(
                    lane < 2 * quarter,
                    pltpu.roll(packed[1], 3 * quarter, 1),
                    pltpu.roll(packed[2], quarter, 1),
                ),
            )
            for k, value in enumerate(packed + [last]):
                to = m * block + k * SUBLANES
                inside[to : to + SUBLANES, LANES:] = value
        depth = len(modes) * block
        high, low = split(inside[:depth, :])
        both = jnp.concatenate([high, low, high], axis=0)
        if first in (0, plan.radix // 2):
            size, table, at = LANES, real_table, real_at
            real_at += size
        else:
            size, table, at = 2 * LANES, full_table, 0
        w_high = table[at : at + size, :depth]
        w_low = table[at : at + size, depth:]
        made = dot(jnp.concatenate([w_high, w_high, w_low], axis=1), both, NN)
        parts_of[part_at : part_at + size, :] = made
        found[first] = (part_at, size > LANES)
        part_at += size
        slot += len(modes)
    for x_l in range(plan.fine_x):
        for piece in range(reps // SUBLANES):
            row = x_l * reps + piece * SUBLANES
            values = []
            for first in range(plan.radix // 2 + 1):
                at, is_full = found[first]
                re = parts_of[at + row : at + row + SUBLANES, :]
                im = None
                if is_full:
                    im = parts_of[at + LANES + row : at + LANES + row + SUBLANES, :]
                value = (re, im)
                if is_full:
                    value = turn(value, 2.0 * math.pi * first * x_l / plan.count)
                values.append(value)
            for xh, value in enumerate(to_real(values)):
                x = xh * plan.fine_x + x_l
                places = [x + 1]
                if x == plan.count - 1:
                    places.append(0)
                if x < 2:
                    places.append(x + 1 + plan.count)
                for place in places:
                    to = place * reps + piece * SUBLANES
                    coarse[to : to + SUBLANES, :] = value

    here = plan.count // steps
    table = jnp.concatenate([stencil[...], stencil[...]], axis=1)
    width = out.shape[2] // steps
    copies = []
    for step in range(steps):
        made = []
        for i in range(here):
            taps = []
            for move in range(4):
                at = (step * here + i + move) * reps
                taps.append(coarse[at : at + reps, :])
            made.append(taps[1])
            made.append((taps[1] + taps[2]) * (9.0 / 16.0) - (taps[0] + taps[3]) * (1.0 / 16.0))
        high, low = split(jnp.concatenate(made, axis=0))
        values = dot(table, jnp.concatenate([high, low], axis=1), NT)
        values = values.reshape(plan.planes + 3, 2 * plan.rows, width)
        for z in range(plan.planes):
            fine[step, 2 * z] = values[z + 1]
            fine[step, 2 * z + 1] = (values[z + 1] + values[z + 2]) * (9.0 / 16.0) - (
                values[z] + values[z + 3]
            ) * (1.0 / 16.0)
        copies.append(
            pltpu.make_async_copy(
                fine.at[step], out.at[:, :, step * width : (step + 1) * width], sent.at[step]
            )
        )
        copies[-1].start(priority=step % 2)
    for copy in copies:
        copy.wait()


def exchanged(values, parts):
    rows = values.shape[0]
    values = values.reshape(parts, 1, rows // parts * LANES)
    values = lax.all_to_all(values, ("gz", "gy"), split_axis=0, concat_axis=0, tiled=True)
    return values.reshape(rows, LANES)


def in_hbm(arrays):
    return [pltpu.with_memory_space_constraint(array, pltpu.HBM) for array in arrays]


def like(arrays):
    return [jax.ShapeDtypeStruct(array.shape, array.dtype) for array in arrays]


def fast_form(plan, charges, kernel):
    f32, bf16 = jnp.float32, jnp.bfloat16
    parts, reps, block = plan.parts, plan.replicas, plan.block
    limit = pltpu.CompilerParams(vmem_limit_bytes=40 * 1024 * 1024)
    me = (lax.axis_index("gz") * plan.ny + lax.axis_index("gy")).reshape(1)

    operands = [charges, kernel] + [jnp.asarray(t) for t in pack_tables(plan)]
    tables = [jnp.asarray(t) for t in plane_tables(plan)]
    packed, *tables = pl.pallas_call(
        functools.partial(pack_kernel, plan, len(tables)),
        out_shape=[jax.ShapeDtypeStruct((parts * plan.sent, LANES), f32)] + like(tables),
        in_specs=[SMEM] + [HBM] * (len(operands) + len(tables)),
        out_specs=[VMEM] * (1 + len(tables)),
        scratch_shapes=room_for(operands) + [pltpu.SemaphoreType.DMA((len(tables),))],
        compiler_params=limit,
        name="pack",
    )(me, *in_hbm(operands), *in_hbm(tables))
    packed = exchanged(packed, parts)

    later = [jnp.asarray(t) for t in unpack_tables(plan) + (stencil_table(plan),)]
    planes = pl.pallas_call(
        functools.partial(plane_kernel, plan),
        out_shape=jax.ShapeDtypeStruct((parts * plan.back, LANES), f32),
        in_specs=[SMEM] + [VMEM] * (1 + len(tables)),
        out_specs=VMEM,
        scratch_shapes=[
            pltpu.VMEM((parts * block, LANES), f32),
            pltpu.VMEM((parts * reps, 2 * LANES), f32),
            pltpu.VMEM((4 * parts, LANES), f32),
            pltpu.VMEM((parts * reps, 2 * LANES), bf16),
            pltpu.VMEM((parts * reps, 2 * LANES), bf16),
            pltpu.VMEM((parts * block, 4 * LANES), bf16),
        ],
        compiler_params=limit,
        name="plane",
    )(me, packed, *tables)
    planes = exchanged(planes, parts)

    steps = plan.radix
    fine_shape = (2 * plan.planes, 2 * plan.rows, 2 * plan.count * reps)
    return pl.pallas_call(
        functools.partial(unpack_kernel, plan, steps),
        out_shape=jax.ShapeDtypeStruct(fine_shape, f32),
        in_specs=[VMEM] * (1 + len(later)),
        out_specs=HBM,
        scratch_shapes=[
            pltpu.VMEM((2 * LANES, 2 * LANES), f32),
            pltpu.VMEM((plan.radix * LANES, 2 * LANES), f32),
            pltpu.VMEM(((plan.count + 3) * reps, 2 * LANES), f32),
            pltpu.VMEM((steps,) + fine_shape[:2] + (fine_shape[2] // steps,), f32),
            pltpu.SemaphoreType.DMA((steps,)),
        ],
        compiler_params=limit,
        name="unpack",
    )(planes, *later)


def extended(block, sides, width):
    for axis, dim in sides:
        count = lax.axis_size(axis)
        forward_pairs = [(i, (i + 1) % count) for i in range(count)]
        backward_pairs = [(target, source) for source, target in forward_pairs]
        low = lax.ppermute(
            lax.slice_in_dim(block, block.shape[dim] - width, None, axis=dim), axis, forward_pairs
        )
        high = lax.ppermute(lax.slice_in_dim(block, 0, width, axis=dim), axis, backward_pairs)
        block = jnp.concatenate([low, block, high], axis=dim)
    return block


def tables_of(count):
    index = jnp.arange(count, dtype=jnp.int32)
    product = index[:, None] * index[None, :] % count
    angle = product.astype(jnp.float32) * (2.0 * math.pi / count)
    return (jnp.cos(angle), jnp.sin(angle))


def along(values, table, axis):
    moved = jnp.tensordot(values, table, axes=((axis,), (0,)), precision=lax.Precision.HIGHEST)
    return jnp.moveaxis(moved, -1, axis)


def forward(spectrum, axis, cosines, sines):
    real_part, imag_part = (spectrum[0], spectrum[1])
    inner = axis - 1
    new_real = along(real_part, cosines, inner) + along(imag_part, sines, inner)
    new_imag = along(imag_part, cosines, inner) - along(real_part, sines, inner)
    return jnp.stack([new_real, new_imag])


def backward(spectrum, axis, cosines, sines):
    real_part, imag_part = (spectrum[0], spectrum[1])
    inner = axis - 1
    count = cosines.shape[0]
    new_real = (along(real_part, cosines, inner) - along(imag_part, sines, inner)) / count
    new_imag = (along(imag_part, cosines, inner) + along(real_part, sines, inner)) / count
    return jnp.stack([new_real, new_imag])


def refine_rim(haloed, axis, count):
    centre = lax.slice_in_dim(haloed, 2, 2 + count, axis=axis)
    before = lax.slice_in_dim(haloed, 1, 1 + count, axis=axis)
    after = lax.slice_in_dim(haloed, 3, 3 + count, axis=axis)
    after_two = lax.slice_in_dim(haloed, 4, 4 + count, axis=axis)
    middle = (9.0 * (centre + after) - (before + after_two)) / 16.0
    stacked = jnp.stack([centre, middle], axis=axis + 1)
    shape = list(centre.shape)
    shape[axis] = 2 * count
    return stacked.reshape(shape)


def refine_loop(coarse, axis):
    before = jnp.roll(coarse, 1, axis)
    after = jnp.roll(coarse, -1, axis)
    after_two = jnp.roll(coarse, -2, axis)
    middle = (9.0 * (coarse + after) - (before + after_two)) / 16.0
    stacked = jnp.stack([coarse, middle], axis=axis + 1)
    shape = list(coarse.shape)
    shape[axis] = 2 * shape[axis]
    return stacked.reshape(shape)


def general_form(charges, kernel):
    planes, rows, count = (kernel.shape[0], kernel.shape[1], kernel.shape[2])
    replicas = charges.shape[2] // count
    grids = charges.reshape(planes, rows, count, replicas)
    cosines, sines = tables_of(count)
    spectrum = jnp.stack([along(grids, cosines, 2), -along(grids, sines, 2)])
    kernel_spec = jnp.stack([along(kernel, cosines, 2), -along(kernel, sines, 2)])
    spectrum, kernel_spec = (
        lax.all_to_all(spectrum, "gy", split_axis=3, concat_axis=2, tiled=True),
        lax.all_to_all(kernel_spec, "gy", split_axis=3, concat_axis=2, tiled=True),
    )
    spectrum = forward(spectrum, 2, cosines, sines)
    kernel_spec = forward(kernel_spec, 2, cosines, sines)
    spectrum, kernel_spec = (
        lax.all_to_all(spectrum, "gz", split_axis=2, concat_axis=1, tiled=True),
        lax.all_to_all(kernel_spec, "gz", split_axis=2, concat_axis=1, tiled=True),
    )
    spectrum = forward(spectrum, 1, cosines, sines)
    kernel_spec = forward(kernel_spec, 1, cosines, sines)
    kernel_real = kernel_spec[0][..., None]
    kernel_imag = kernel_spec[1][..., None]
    product_real = spectrum[0] * kernel_real - spectrum[1] * kernel_imag
    product_imag = spectrum[1] * kernel_real + spectrum[0] * kernel_imag
    spectrum = backward(jnp.stack([product_real, product_imag]), 1, cosines, sines)
    spectrum = lax.all_to_all(spectrum, "gz", split_axis=1, concat_axis=2, tiled=True)
    spectrum = backward(spectrum, 2, cosines, sines)
    spectrum = lax.all_to_all(spectrum, "gy", split_axis=2, concat_axis=3, tiled=True)
    potential = (along(spectrum[0], cosines, 2) - along(spectrum[1], sines, 2)) / count
    haloed = extended(potential, (("gz", 0), ("gy", 1)), 2)
    result = refine_rim(haloed, 0, planes)
    result = refine_rim(result, 1, rows)
    result = refine_loop(result, 2)
    return result.reshape(2 * planes, 2 * rows, 2 * count * replicas)


def per_device(nz, ny, charges, kernel):
    planes, rows, count = kernel.shape
    replicas = charges.shape[2] // count
    sizes = (planes, rows, count, replicas, nz, ny)
    if Plan.fits(*sizes):
        return fast_form(Plan(*sizes), charges, kernel)
    return general_form(charges, kernel)


def solution(mesh):
    placed = (P("gz", "gy", None), P("gz", "gy", None))
    sizes = (mesh.shape["gz"], mesh.shape["gy"])
    return jax.shard_map(
        functools.partial(per_device, *sizes),
        mesh=mesh,
        in_specs=placed,
        out_specs=P("gz", "gy", None),
        check_vma=False,
    )
```
